32 devices in a mesh: gx: 4 (over x, core), gy: 8 (over z, y).
Axes of the slice: x: 2, y: 2, z: 4, core: 2. Of those that a mesh axis runs over, the one named last changes fastest.
Arguments:
- log_crit: float32 [512, 512, 128], P('gx', 'gy'), may hold values from -4 to 4
- col_bins: int32 [512, 512, 4], P('gx', 'gy'), may hold values from 0 to 127
- rate_table: bfloat16 [128, 64], replicated, may hold values from 0.0039978027 to 0.059814453
- tile_mask: int32 [16, 16, 4], P('gx', 'gy'), may hold values from 0 to 1, as said below
- tile_route: int32 [16, 16, 4], P('gx', 'gy'), may hold values from 0 to 7, as said below
- filt_x: float32 [512], replicated, may hold values from 0.1 to 1, as said below
- filt_y: float32 [512], replicated, may hold values from 0.1 to 1, as said below
Outputs:
- recomb: float32 [512, 512, 128], P('gx', 'gy')
- smoothed: float32 [512, 512, 128], P('gx', 'gy')
- load: float32 [4, 8], P('gx', 'gy')
The draws below stay inside these ranges and needn't reach their ends.
Inputs may be any that keep to these rules, and one draw needn't show every extreme that they name: `tile_mask`: tiles form blocks of 4 x 2 x 4 (indices a // 4, b // 2); among the blocks with the same a // 4, some block has all 32 tiles active. `tile_route`: counting only tiles with tile_mask 1: among the blocks with the same a // 4 at most 16 active tiles share a route, and in every draw some such row of blocks gives every route exactly 16; at most 4 active tiles of one block share a route, and in every draw some block has 4 that do. filt_x[m] == filt_x[512 - m] for 0 < m < 512. filt_y[n] == filt_y[512 - n] for 0 < n < 512.
All inputs are finite; a program needn't handle non-finite values.
Results may differ from the reference program's by a relative error of at most 0.0003.
Values sent between devices are 32-bit elements; how exact they have to be, the bound alone decides.
A program may use at most 128 MiB of HBM per device.

```python
import math
import jax
import jax.numpy as jnp
from jax import lax

TE = 32
TX = 4
TY = 2
TZ = 4
BINS = 128
NODES = 64
RECV = 16
NX = 512
NY = 512
NZ = 128
N_GX = 4
N_GY = 8


def tile_plan(key):
    base_key = jax.random.fold_in(key, 11)
    k_count, k_busy, k_row, k_perm, k_spare = jax.random.split(base_key, 5)
    tiles_block = TX * TY * TZ
    half_tiles = tiles_block // 2
    quarter_tiles = tiles_block // 4
    pair_cap = tiles_block // N_GY
    counts = jax.random.randint(k_count, (N_GX, N_GY), quarter_tiles, half_tiles)
    busiest = jax.random.randint(k_busy, (N_GX,), 0, N_GY)
    full_row = jax.random.randint(k_row, (), 0, N_GX)
    column_ids = jnp.arange(N_GY)[None, :]
    counts = jnp.where(jnp.arange(N_GX)[:, None] == full_row, half_tiles, counts)
    counts = jnp.where(column_ids == busiest[:, None], tiles_block, counts)
    counts = jnp.where(column_ids == (busiest[:, None] + 1) % N_GY, 0, counts)
    perm_keys = jax.random.split(k_perm, N_GX * N_GY)
    tile_ranks = jax.vmap(lambda sub_key: jax.random.permutation(sub_key, tiles_block))(perm_keys).reshape(N_GX, N_GY, tiles_block)
    active = (tile_ranks < counts[:, :, None]).astype(jnp.int32)
    row_flags = active.reshape(N_GX, N_GY * tiles_block)
    before = jnp.cumsum(row_flags, axis=1) - row_flags
    chosen = (before // pair_cap % N_GY).reshape(N_GX, N_GY, tiles_block)
    spare_route = jax.random.randint(k_spare, (N_GX, N_GY, tiles_block), 0, N_GY)
    routes = jnp.where(active == 1, chosen, spare_route).astype(jnp.int32)
    return (lay_out(active), lay_out(routes))


def lay_out(values):
    shaped = values.reshape(N_GX, N_GY, TX, TY, TZ).transpose(0, 2, 1, 3, 4)
    return shaped.reshape(N_GX * TX, N_GY * TY, TZ)


def window_draw(key, length):
    half = length // 2 + 1
    values = jnp.exp(jax.random.uniform(key, (half,), jnp.float32, math.log(0.1), 0.0))
    indices = jnp.arange(length)
    folded = jnp.minimum(indices, length - indices)
    return values[folded].astype(jnp.float32)


def draw_tile_mask(key, part):
    return tile_plan(key)[0]


def draw_tile_route(key, part):
    return tile_plan(key)[1]


def draw_filt_x(key, part):
    return window_draw(jax.random.fold_in(key, 21), NX)


def draw_filt_y(key, part):
    return window_draw(jax.random.fold_in(key, 23), NY)


def plant(result, own_key, smallest, largest):
    place = [jax.random.randint(jax.random.fold_in(own_key, axis), (), 0, length) for axis, length in enumerate(result.shape)]
    widest = result.shape.index(max(result.shape))
    beside = place[:widest] + [(place[widest] + 1) % result.shape[widest]] + place[widest + 1:]
    return result.at[tuple(place)].set(smallest).at[tuple(beside)].set(largest)


def block_scale(stream_key, dims, shards, low, largest):
    loudness = 1.0
    for position, parts in shards:
        heights = jax.random.uniform(jax.random.fold_in(jax.random.fold_in(stream_key, 6), position), (parts,), jnp.float32, low / len(shards), largest / len(shards))
        loudness = loudness * jnp.repeat(jnp.exp(heights), dims[position] // parts).reshape((-1,) + (1,) * (len(dims) - 1 - position))
    return loudness


def normal_values(own_key, shape, scale, reach, cuts=(), kind=jnp.bfloat16):
    drawn = scale * jax.random.normal(own_key, shape, jnp.float32)
    if cuts:
        drawn = drawn * block_scale(own_key, shape, cuts, -0.22, 0.18)
    return jnp.clip(drawn, -reach, reach).astype(kind)


def setup_inputs(seed: int = 0) -> dict:
    key_of = jax.random.split(jax.random.key(seed), 8)
    return {
        "log_crit": normal_values(key_of[0], (NX, NY, NZ), 1.0, 4.0, ((0, 4), (1, 8)), jnp.float32),
        "col_bins": plant(jax.random.randint(key_of[1], (NX, NY, TZ), 0, BINS), jax.random.fold_in(key_of[1], 1), 0, BINS - 1).astype(jnp.int32),
        "rate_table": jnp.clip(jnp.exp(jax.random.uniform(key_of[2], (BINS, NODES), jnp.float32, math.log(0.0039978027), math.log(0.059814453))), 0.0039978027, 0.059814453).astype(jnp.bfloat16),
        "tile_mask": draw_tile_mask(jax.random.fold_in(key_of[7], 71), 0),
        "tile_route": draw_tile_route(jax.random.fold_in(key_of[7], 71), 0),
        "filt_x": draw_filt_x(jax.random.fold_in(key_of[7], 71), 0),
        "filt_y": draw_filt_y(jax.random.fold_in(key_of[7], 71), 0),
    }


steepness = 3.0


def reference(log_crit, col_bins, rate_table, tile_mask, tile_route, filt_x, filt_y):
    size_x, size_y, size_z = log_crit.shape
    rows_x = N_GX * TX
    rows_y = N_GY * TY
    tile_cells = log_crit.reshape(rows_x, TE, rows_y, TE, TZ, TE).transpose(0, 2, 4, 1, 3, 5).reshape(-1, TE, TE, TE)
    tile_bins = col_bins.reshape(rows_x, TE, rows_y, TE, TZ).transpose(0, 2, 4, 1, 3).reshape(-1, TE, TE)
    live_flags = tile_mask.reshape(-1)
    table_f32 = rate_table.astype(jnp.float32)
    node_grid = -2.5 + 5.0 * jnp.arange(NODES, dtype=jnp.float32) / (NODES - 1)

    def tile_value(operands):
        field, bin_cols, is_live = operands
        table_rows = table_f32[bin_cols]

        def active(unused):
            cutoff = jax.nn.sigmoid((field[..., None] - node_grid) * steepness)
            return jnp.sum(cutoff * table_rows[:, :, None, :], axis=-1)

        def quiet(unused):
            return jnp.zeros_like(field)

        return lax.cond(is_live == 1, active, quiet, 0)

    values = lax.map(tile_value, (tile_cells, tile_bins, live_flags))
    tile_mean = jnp.mean(values.reshape(values.shape[0], -1), axis=1).reshape(rows_x, rows_y, TZ)
    onehot = (tile_route[..., None] == jnp.arange(N_GY)).astype(jnp.float32)
    per_row = jnp.einsum('abt,abtg->ag', tile_mean.astype(jnp.float32), onehot)
    load = jnp.sum(per_row.reshape(N_GX, TX, N_GY), axis=1) / RECV
    recomb = values.reshape(rows_x, rows_y, TZ, TE, TE, TE).transpose(0, 3, 1, 4, 2, 5).reshape(size_x, size_y, size_z)
    gain_plane = filt_x[:, None, None] * filt_y[None, :, None]
    z_block = 16 if size_z % 16 == 0 else size_z
    blocks = recomb.reshape(size_x, size_y, size_z // z_block, z_block).transpose(2, 0, 1, 3)

    def smooth_block(block):
        spectrum = jnp.fft.fft2(block, axes=(0, 1))
        return jnp.real(jnp.fft.ifft2(spectrum * gain_plane, axes=(0, 1))).astype(jnp.float32)

    smoothed = lax.map(smooth_block, blocks).transpose(1, 2, 0, 3).reshape(size_x, size_y, size_z)
    return recomb, smoothed, load
```

```python
import functools
import math

import jax
import jax.numpy as jnp
from jax import lax
from jax.experimental import pallas as pl
from jax.experimental.pallas import tpu as pltpu
from jax.sharding import PartitionSpec as P

steepness = 3.0
vmem_grant = 60 * 1024 * 1024
MESH = pl.DeviceIdType.MESH
levels = 4


def node_growth(nodes):
    return [math.exp(steepness * (-2.5 + 5.0 * q / (nodes - 1))) for q in range(nodes // 2, nodes)]


def join(left, right):
    num_left, den_left = left
    num_right, den_right = right
    return (num_left * den_right + num_right * den_left, den_left * den_right)


def integral(field, i, growth, coef_a, coef_b):
    pairs = len(growth)
    v = jnp.exp(field * steepness)
    y = v + jnp.exp(field * -steepness)
    total = None
    for first in range(0, pairs, 4):
        terms = []
        for p in range(first, min(first + 4, pairs)):
            num = coef_a[i, pl.ds(p, 1), :] * v + coef_b[i, pl.ds(p, 1), :]
            terms.append((num, y + (growth[p] + 1.0 / growth[p])))
        while len(terms) > 1:
            terms = [
                join(terms[i], terms[i + 1]) if i + 1 < len(terms) else terms[i]
                for i in range(0, len(terms), 2)
            ]
        part = terms[0][0] * (1.0 / terms[0][1])
        total = part if total is None else total + part
    return total


def eval_kernel(
    growth, tiles, field_ref, bins_ref, live_ref, table_ref, rise_ref, recomb_ref, zfirst_ref,
    sums_ref, turned, values, coef_a, coef_b,
):
    cells_x, rows, depth_all = field_ref.shape
    edge = depth_all // tiles
    pairs = len(growth)
    bins_total = table_ref.shape[1]
    for row in range(rows):
        turned[row] = field_ref[:, row, :].T

    def gather(i, carry):
        levels = lax.broadcasted_iota(jnp.int32, (bins_total, cells_x), 0)
        onehot = jnp.where(levels == bins_ref[pl.ds(i, 1), :], 1.0, 0.0).astype(jnp.bfloat16)
        rows_here = jnp.dot(table_ref[...], onehot, preferred_element_type=jnp.float32)
        rows_here = rows_here * live_ref[pl.ds(i, 1), :]
        upper, lower = rows_here[:pairs], rows_here[pairs:]
        coef_a[i] = upper + lower
        coef_b[i] = upper * rise_ref[1] + lower * rise_ref[0]
        return carry

    def step(i, carry):
        row, tile = i // tiles, i % tiles
        span = pl.ds(pl.multiple_of(tile * edge, edge), edge)
        out = integral(turned[row, span, :], i, growth, coef_a, coef_b)
        values[row, span, :] = out
        sums_ref[pl.ds(i, 1), :] = jnp.sum(out, axis=0, keepdims=True)
        return carry

    lax.fori_loop(0, rows * tiles, gather, 0, unroll=8)
    lax.fori_loop(0, rows * tiles, step, 0)
    for row in range(rows):
        recomb_ref[:, row, :] = values[row].T
        zfirst_ref[:, row, :] = values[row]


def evaluate(log_crit, bins, live, table, growth, tiles):
    cells_x, cells_y, depth_all = log_crit.shape
    rows = 8
    nodes, bins_total = table.shape
    ends = jnp.array([growth, [1.0 / e for e in growth]], jnp.float32)
    rise = jnp.broadcast_to(ends[:, :, None], (2, nodes // 2, cells_x))
    return pl.pallas_call(
        functools.partial(eval_kernel, growth, tiles),
        grid=(cells_y // rows,),
        in_specs=[
            pl.BlockSpec((cells_x, rows, depth_all), lambda j: (0, j, 0)),
            pl.BlockSpec((rows * tiles, cells_x), lambda j: (j, 0)),
            pl.BlockSpec((rows * tiles, cells_x), lambda j: (j, 0)),
            pl.BlockSpec((nodes, bins_total), lambda j: (0, 0)),
            pl.BlockSpec((2, nodes // 2, cells_x), lambda j: (0, 0, 0)),
        ],
        out_specs=[
            pl.BlockSpec((cells_x, rows, depth_all), lambda j: (0, j, 0)),
            pl.BlockSpec((depth_all, rows, cells_x), lambda j: (0, j, 0)),
            pl.BlockSpec((rows * tiles, cells_x), lambda j: (j, 0)),
        ],
        out_shape=[
            jax.ShapeDtypeStruct((cells_x, cells_y, depth_all), jnp.float32),
            jax.ShapeDtypeStruct((depth_all, cells_y, cells_x), jnp.float32),
            jax.ShapeDtypeStruct((cells_y * tiles, cells_x), jnp.float32),
        ],
        scratch_shapes=[
            pltpu.VMEM((rows, depth_all, cells_x), jnp.float32),
            pltpu.VMEM((rows, depth_all, cells_x), jnp.float32),
            pltpu.VMEM((rows * tiles, nodes // 2, cells_x), jnp.float32),
            pltpu.VMEM((rows * tiles, nodes // 2, cells_x), jnp.float32),
        ],
        compiler_params=pltpu.CompilerParams(vmem_limit_bytes=vmem_grant),
        name="evaluate",
    )(log_crit, bins, live, table, rise)


def halves(value):
    high = value.astype(jnp.bfloat16)
    return high, (value - high.astype(jnp.float32)).astype(jnp.bfloat16)


def outer_halves(value):
    high = lax.reduce_precision(value, 8, 7)
    low = lax.reduce_precision(value - high, 8, 7)
    return high.astype(jnp.bfloat16), low.astype(jnp.bfloat16)


def dot3(a_high, a_low, b_high, b_low):
    dot = functools.partial(jnp.dot, preferred_element_type=jnp.float32)
    return dot(a_high, b_high) + (dot(a_high, b_low) + dot(a_low, b_high))


def share_kernel(span_x, span_y, mine, out, send_sem, recv_sem, own_sem):
    devices = span_x * span_y
    gx, gy = lax.axis_index("gx"), lax.axis_index("gy")
    me = gx * span_y + gy

    def each_peer(act):
        def body(n, carry):
            i = lax.rem(gx + n // span_y, span_x)
            j = lax.rem(gy + n % span_y, span_y)
            act({"gx": i, "gy": j})
            return carry

        lax.fori_loop(1, devices, body, 0)

    barrier = pltpu.get_barrier_semaphore()
    each_peer(lambda peer: pl.semaphore_signal(barrier, inc=1, device_id=peer, device_id_type=MESH))
    own = pltpu.make_async_copy(mine, out.at[me], own_sem)
    own.start()
    pl.semaphore_wait(barrier, devices - 1)

    def send(peer):
        pltpu.make_async_remote_copy(
            src_ref=mine,
            dst_ref=out.at[me],
            send_sem=send_sem,
            recv_sem=recv_sem,
            device_id=peer,
            device_id_type=MESH,
        ).start()

    each_peer(send)
    own.wait()
    some = out.at[pl.ds(0, devices - 1)]
    pltpu.make_async_copy(some, some, send_sem).wait()
    pltpu.make_async_copy(some, some, recv_sem).wait()


def share(mine, span_x, span_y):
    inside = pl.BlockSpec(memory_space=pltpu.VMEM)
    return pl.pallas_call(
        functools.partial(share_kernel, span_x, span_y),
        in_specs=[inside],
        out_specs=inside,
        out_shape=jax.ShapeDtypeStruct((span_x * span_y,) + mine.shape, mine.dtype),
        scratch_shapes=[pltpu.SemaphoreType.DMA] * 3,
        compiler_params=pltpu.CompilerParams(collective_id=1, has_side_effects=True),
        name="share",
    )(mine)


def exchange_kernel(
    span_x, span_y, edge, zfirst, loads, source_ref, place_ref, cy_high, cy_low, cx_high, cx_low,
    out, load_parts, own, line, packed, arrived, stage, unpack_stage, high, low,
    first_send, first_recv, first_own, line_send, line_recv, far_send, far_recv,
    back_send, back_recv, back_own, load_sems,
):
    steps, group, cells_y, cells_x = zfirst.shape
    size_y, size_x = high.shape
    part = group // span_x
    rows = part * cells_y
    per = 128 // edge
    packs = packed.shape[1]
    tiles_x = size_x // edge
    lane_blocks = size_x // 128
    tiles = source_ref.shape[1]
    block = 128
    gx, gy = lax.axis_index("gx"), lax.axis_index("gy")
    level, w = gy // part, lax.rem(gy, part)
    half, side = level // 2, lax.rem(level, 2)
    mate = 2 * half + 1 - side
    me = gx * part + w
    is_middle = (level == 1) | (level == 2)
    is_end = (level == 0) | (level == 3)

    def at(i, j):
        return {"gx": i, "gy": j}

    def place(ref, s, i, j):
        return ref.at[
            s,
            pl.ds(pl.multiple_of(j * cells_y, cells_y), cells_y),
            pl.ds(pl.multiple_of(i * cells_x, cells_x), cells_x),
        ]

    def each_of_level(act):
        def body(n, carry):
            act(lax.rem(gx + n // part, span_x), lax.rem(w + n % part, part))
            return carry

        lax.fori_loop(1, group, body, 0)

    def every_peer(act):
        def body(n, carry):
            act(lax.rem(gx + n // span_y, span_x), lax.rem(gy + n % span_y, span_y))
            return carry

        lax.fori_loop(1, span_x * span_y, body, 0)

    barrier = pltpu.get_barrier_semaphore()
    every_peer(
        lambda i, j: pl.semaphore_signal(barrier, inc=1, device_id=at(i, j), device_id_type=MESH)
    )
    for s in range(steps):
        pltpu.make_async_copy(zfirst.at[s, me], place(own, s, gx, w), first_own.at[s]).start()
    pl.semaphore_wait(barrier, span_x * span_y - 1)

    def first(s):
        def act(i, j):
            pltpu.make_async_remote_copy(
                src_ref=zfirst.at[s, i * part + j],
                dst_ref=place(own, s, gx, w),
                send_sem=first_send.at[s],
                recv_sem=first_recv.at[s],
                device_id=at(i, level * part + j),
                device_id_type=MESH,
            ).start()

        each_of_level(act)

    def send_back(s):
        def act(i, j):
            pltpu.make_async_remote_copy(
                src_ref=place(line, s, i, j),
                dst_ref=out.at[s, me],
                send_sem=back_send.at[s],
                recv_sem=back_recv.at[s],
                device_id=at(i, level * part + j),
                device_id_type=MESH,
            ).start()

        each_of_level(act)
        pltpu.make_async_copy(place(line, s, gx, w), out.at[s, me], back_own.at[s]).start()

    def to_mate(source, s):
        return pltpu.make_async_remote_copy(
            src_ref=source.at[s],
            dst_ref=line.at[s],
            send_sem=line_send.at[s],
            recv_sem=line_recv.at[s],
            device_id=at(gx, mate * part + w),
            device_id_type=MESH,
        )

    def to_far(s):
        return pltpu.make_async_remote_copy(
            src_ref=packed.at[s],
            dst_ref=arrived.at[s],
            send_sem=far_send.at[s],
            recv_sem=far_recv.at[s],
            device_id=at(gx, (3 - level) * part + w),
            device_id_type=MESH,
        )

    def wait_others(sem, s):
        some = zfirst.at[0, pl.ds(0, group - 1)]
        pltpu.make_async_copy(some, some, sem.at[s]).wait()

    def wait_own(sem, s):
        one = zfirst.at[0, 0]
        pltpu.make_async_copy(one, one, sem.at[s]).wait()

    def wait_plane(sem, s):
        pltpu.make_async_copy(own.at[s], own.at[s], sem.at[s]).wait()

    def wait_packed(sem, s):
        pltpu.make_async_copy(packed.at[s], packed.at[s], sem.at[s]).wait()

    own_load = pltpu.make_async_copy(loads.at[gy], load_parts.at[gy], load_sems.at[2])
    own_load.start()

    def send_load(n, carry):
        j = lax.rem(gy + n, span_y)
        pltpu.make_async_remote_copy(
            src_ref=loads.at[j],
            dst_ref=load_parts.at[gy],
            send_sem=load_sems.at[0],
            recv_sem=load_sems.at[1],
            device_id=at(gx, j),
            device_id_type=MESH,
        ).start()
        return carry

    lax.fori_loop(1, span_y, send_load, 0)

    def begin(s, carry):
        first(s)
        return carry

    lax.fori_loop(0, steps, begin, 0)

    lane = lax.broadcasted_iota(jnp.int32, (edge, 128), 1)
    for r in range(per):
        unpack_stage[r] = jnp.zeros((edge, 128), jnp.float32)

    def rows_at(start, count):
        return pl.ds(pl.multiple_of(start, count), count)

    def turns(value):
        return [value if r == 0 else pltpu.roll(value, r * edge, 1) for r in range(per)]

    def pack(s):
        def fill(n, carry):
            down, across = n // lane_blocks, pl.ds(pl.multiple_of(n % lane_blocks * 128, 128), 128)
            chunk = rows_at(down * edge, edge)
            strip = rows // edge * lane_blocks
            for r, value in enumerate(turns(own[s, chunk, across])):
                stage[(side * strip + n) * per + r] = value
            for r, value in enumerate(turns(line[s, chunk, across])):
                stage[((1 - side) * strip + n) * per + r] = value
            return carry

        lax.fori_loop(0, rows // edge * lane_blocks, fill, 0)
        t = s // (steps // tiles)

        def one(g, carry):
            total = None
            for q in range(per):
                piece = stage[source_ref[half, t, g * per + q]]
                total = piece if total is None else jnp.where(lane >= q * edge, piece, total)
            packed[s, g] = total
            return carry

        lax.fori_loop(0, packs, one, 0)

    def unpack(s):
        def fill(g, carry):
            for r, value in enumerate(turns(arrived[s, g])):
                unpack_stage[(g + 1) * per + r] = value
            return carry

        lax.fori_loop(0, packs, fill, 0)
        t = s // (steps // tiles)

        def one(n, carry):
            down, block_x = n // lane_blocks, lax.rem(n, lane_blocks)
            total = None
            for q in range(per):
                piece = unpack_stage[place_ref[1 - half, t, n * per + q]]
                total = piece if total is None else jnp.where(lane >= q * edge, piece, total)
            to = (
                rows_at((1 - half) * 2 * rows + down * edge, edge),
                rows_at(block_x * 128, 128),
            )
            high[to], low[to] = halves(total)
            return carry

        lax.fori_loop(0, 2 * rows // edge * lane_blocks, one, 0)

    def split(source, s, which):
        def one(r, carry):
            to = rows_at(which * rows + r * block, block)
            high[to, :], low[to, :] = halves(source[s, rows_at(r * block, block), :])
            return carry

        lax.fori_loop(0, rows // block, one, 0)

    def along_y(which, r):
        chunk = rows_at(which * rows + r * block, block)
        return dot3(cy_high[chunk, :], cy_low[chunk, :], high[...], low[...])

    def along_x(value):
        return dot3(*halves(value), cx_high[...], cx_low[...])

    def middle_first(s):
        wait_own(first_own, s)
        wait_others(first_recv, s)
        wait_plane(line_recv, s)
        pack(s)
        to_far(s).start()

    def middle_second(s):
        split(own, s, level)
        split(line, s, mate)
        wait_packed(far_recv, s)
        unpack(s)

        def for_mate(r, carry):
            own[s, rows_at(r * block, block), :] = along_y(mate, r)
            return carry

        lax.fori_loop(0, rows // block, for_mate, 0)
        to_mate(own, s).start()

        def for_me(r, carry):
            line[s, rows_at(r * block, block), :] = along_x(along_y(level, r))
            return carry

        lax.fori_loop(0, rows // block, for_me, 0)
        send_back(s)

    ahead = min(2, steps - 1)

    @pl.when(is_middle)
    def _():
        def body(i, carry):
            @pl.when(i < steps)
            def _():
                middle_first(i)

            @pl.when(i >= ahead)
            def _():
                middle_second(i - ahead)

            return carry

        lax.fori_loop(0, steps + ahead, body, 0)

        def drain(s, carry):
            wait_packed(far_send, s)
            wait_plane(line_send, s)
            return carry

        lax.fori_loop(0, steps, drain, 0)

    @pl.when(is_end)
    def _():
        def feed(s, carry):
            wait_own(first_own, s)
            wait_others(first_recv, s)
            to_mate(own, s).start()
            return carry

        lax.fori_loop(0, steps, feed, 0)

        def body(s, carry):
            wait_plane(line_recv, s)

            def for_me(r, carry):
                line[s, rows_at(r * block, block), :] = along_x(line[s, rows_at(r * block, block), :])
                return carry

            lax.fori_loop(0, rows // block, for_me, 0)
            send_back(s)
            return carry

        lax.fori_loop(0, steps, body, 0)

        def drain(s, carry):
            wait_plane(line_send, s)
            return carry

        lax.fori_loop(0, steps, drain, 0)

    some_loads = loads.at[pl.ds(0, span_y - 1)]
    pltpu.make_async_copy(some_loads, some_loads, load_sems.at[0]).wait()
    pltpu.make_async_copy(some_loads, some_loads, load_sems.at[1]).wait()
    own_load.wait()

    def finish(s, carry):
        wait_others(first_send, s)
        wait_others(back_send, s)
        wait_own(back_own, s)
        wait_others(back_recv, s)
        return carry

    lax.fori_loop(0, steps, finish, 0)


def exchange(
    slots, collective, zfirst, loads, source, position, cy_high, cy_low, cx_high, cx_low, span_x,
    span_y, edge,
):
    steps, group, cells_y, cells_x = zfirst.shape
    size_y, size_x = cy_high.shape[0], cx_high.shape[0]
    rows = size_y // levels
    packs = slots * edge // 128
    anywhere = pl.BlockSpec(memory_space=pl.ANY)
    inside = pl.BlockSpec(memory_space=pltpu.VMEM)
    scalars = pl.BlockSpec(memory_space=pltpu.SMEM)
    planes = pltpu.VMEM((steps, rows, size_x), jnp.float32)
    packing = pltpu.VMEM((steps, packs, edge, 128), jnp.float32)
    sems = pltpu.SemaphoreType.DMA((steps,))
    return pl.pallas_call(
        functools.partial(exchange_kernel, span_x, span_y, edge),
        in_specs=[anywhere] * 2 + [scalars] * 2 + [inside] * 4,
        out_specs=[anywhere] * 2,
        out_shape=[
            jax.ShapeDtypeStruct(zfirst.shape, jnp.float32),
            jax.ShapeDtypeStruct(loads.shape, jnp.float32),
        ],
        scratch_shapes=[
            planes,
            planes,
            packing,
            packing,
            pltpu.VMEM((2 * rows * size_x // edge // edge, edge, 128), jnp.float32),
            pltpu.VMEM((128 // edge * (packs + 1), edge, 128), jnp.float32),
            pltpu.VMEM((size_y, size_x), jnp.bfloat16),
            pltpu.VMEM((size_y, size_x), jnp.bfloat16),
        ]
        + [sems] * 10
        + [pltpu.SemaphoreType.DMA((3,))],
        compiler_params=pltpu.CompilerParams(
            collective_id=collective, has_side_effects=True, vmem_limit_bytes=vmem_grant
        ),
        name=f"exchange{slots}",
    )(zfirst, loads, source, position, cy_high, cy_low, cx_high, cx_low)


def slot_tables(masks, edge):
    halves_count = 2
    flat = masks.reshape(halves_count, -1, masks.shape[2]).transpose(0, 2, 1)
    slots = flat.shape[2]
    before = jnp.triu(jnp.ones((slots, slots), jnp.bfloat16), 1)
    rank = jnp.dot(flat.astype(jnp.bfloat16), before, preferred_element_type=jnp.float32)
    rank = rank.astype(jnp.int32)
    per = 128 // edge
    indices = jnp.arange(slots, dtype=jnp.int32)
    shifted = (indices % per - rank) % per
    position = jnp.where(flat == 1, rank, -1)
    place = jnp.where(flat == 1, (rank // per + 1) * per + shifted, 0)
    from_place = indices // per * per + (rank - indices) % per
    source = jnp.sum(
        jnp.where(position[:, :, None, :] == indices[:, None], from_place[:, :, None, :], 0), axis=3
    )
    most = jnp.max(jnp.sum(flat, axis=2))
    return source, place, most


def turn_kernel(source_ref, out_ref):
    for row in range(source_ref.shape[1]):
        out_ref[:, row, :] = source_ref[:, row, :].T


def turn(source):
    depth_all, cells_y, cells_x = source.shape
    rows = 8
    return pl.pallas_call(
        turn_kernel,
        grid=(cells_y // rows,),
        in_specs=[pl.BlockSpec((depth_all, rows, cells_x), lambda j: (0, j, 0))],
        out_specs=pl.BlockSpec((cells_x, rows, depth_all), lambda j: (0, j, 0)),
        out_shape=jax.ShapeDtypeStruct((cells_x, cells_y, depth_all), jnp.float32),
        name="turn",
    )(source)


def wave_freq(length):
    half = length // 2
    return jnp.concatenate(
        [jnp.arange(half + 1, dtype=jnp.int32), jnp.arange(1, half, dtype=jnp.int32)]
    )


def wave_table(length):
    half = length // 2
    indices = jnp.arange(length, dtype=jnp.int32)
    turns = indices[:, None] * wave_freq(length)[None, :] % length
    angles = 2.0 * math.pi / length * turns.astype(jnp.float32)
    shift = jnp.where(indices < half + 1, 0.0, math.pi / 2)[None, :]
    return lax.optimization_barrier(jnp.cos(angles - shift))


def circulant(gain, table):
    length = gain.shape[0]
    half = length // 2
    freq = wave_freq(length)
    weight = jnp.concatenate([gain[: half + 1], gain[1:half]])
    doubled = jnp.where((freq == 0) | (freq == half), 1.0, 2.0).astype(jnp.float32)
    scaled = lax.optimization_barrier(table * (weight * doubled / length))
    return lax.dot_general(
        scaled, table, (((1,), (1,)), ((), ())), precision=lax.Precision.HIGHEST
    )


def on_device(log_crit, col_bins, rate_table, tile_mask, tile_route, filt_x, filt_y):
    blocks_x, blocks_y, tiles = tile_mask.shape
    cells_x, cells_y, depth_all = log_crit.shape
    edge = cells_x // blocks_x
    span_x, span_y = lax.axis_size("gx"), lax.axis_size("gy")
    devices = span_x * span_y
    nodes = rate_table.shape[1]
    half = nodes // 2

    bins = col_bins.transpose(1, 2, 0).reshape(cells_y * tiles, cells_x)
    live = (tile_mask == 1).astype(jnp.float32).transpose(1, 2, 0)
    live = jnp.broadcast_to(
        live[:, None, :, :, None], (blocks_y, edge, tiles, blocks_x, edge)
    ).reshape(cells_y * tiles, cells_x)
    table = jnp.concatenate([rate_table[:, half:], rate_table[:, half - 1 :: -1]], axis=1).T

    recomb, zfirst, sums = evaluate(log_crit, bins, live, table, node_growth(nodes), tiles)

    tile_means = jnp.sum(
        sums.reshape(blocks_y, edge, tiles, blocks_x, edge), axis=(1, 4)
    ) / (edge * edge * edge)
    route = tile_route.transpose(1, 2, 0)
    capacity = blocks_x * blocks_y * tiles // 2
    route_ids = jnp.arange(span_y, dtype=jnp.int32)
    contribution = (
        jnp.sum(
            jnp.where(route[..., None] == route_ids, tile_means[..., None], 0.0), axis=(0, 1, 2)
        )
        / capacity
    )
    table_x = wave_table(filt_x.shape[0])
    table_y = table_x if filt_y.shape == filt_x.shape else wave_table(filt_y.shape[0])
    mine = jnp.pad((tile_mask == 1).astype(jnp.int32).reshape(1, -1), ((0, 7), (0, 128 - blocks_x * blocks_y * tiles)))
    masks = share(mine, span_x, span_y)[:, 0, : blocks_x * blocks_y * tiles]
    masks = masks.reshape(span_x, span_y, blocks_x, blocks_y, tiles).transpose(1, 3, 0, 2, 4)
    masks = masks.reshape(span_y * blocks_y, span_x * blocks_x, tiles)
    source, position, most = slot_tables(masks, edge)
    every = position.shape[2]
    few = every * 19 // 32
    group = devices // levels
    operands = (
        zfirst.reshape(depth_all // group, group, cells_y, cells_x),
        jnp.broadcast_to(contribution[:, None, None], (span_y, 8, 128)),
        source, position,
        *outer_halves(circulant(filt_y, table_y)), *outer_halves(circulant(filt_x, table_x)),
    )

    def run(slots, collective):
        return lambda *args: exchange(slots, collective, *args, span_x, span_y, edge)

    back, load_parts = lax.cond(most <= few, run(few, 2), run(every, 3), *operands)
    device_load = jnp.sum(load_parts[:, 0, 0])
    smoothed = turn(back.reshape(depth_all, cells_y, cells_x))
    return (recomb, smoothed, device_load.reshape(1, 1))


def solution(mesh):
    placed = (
        P("gx", "gy", None),
        P("gx", "gy", None),
        P(),
        P("gx", "gy", None),
        P("gx", "gy", None),
        P(),
        P(),
    )
    return jax.shard_map(
        on_device,
        mesh=mesh,
        in_specs=placed,
        out_specs=(P("gx", "gy", None), P("gx", "gy", None), P("gx", "gy")),
        check_vma=False,
    )
```

```python
import functools
import math

import jax
import jax.numpy as jnp
import numpy as np
from jax import lax
from jax.experimental import pallas as pl
from jax.experimental.pallas import tpu as pltpu
from jax.sharding import PartitionSpec as P

steepness = 3.0
vmem_grant = 60 * 1024 * 1024
MESH = pl.DeviceIdType.MESH
levels = 4


def node_growth(nodes):
    return [math.exp(steepness * (-2.5 + 5.0 * q / (nodes - 1))) for q in range(nodes // 2, nodes)]


def join(left, right):
    num_left, den_left = left
    num_right, den_right = right
    return (num_left * den_right + num_right * den_left, den_left * den_right)


def integral(field, growth, coef_a, coef_b):
    pairs = len(growth)
    v = jnp.exp(field * steepness)
    y = v + jnp.exp(field * -steepness)
    total = None
    for first in range(0, pairs, 4):
        terms = []
        for p in range(first, min(first + 4, pairs)):
            num = coef_a(p) * v + coef_b(p)
            terms.append((num, y + (growth[p] + 1.0 / growth[p])))
        while len(terms) > 1:
            terms = [
                join(terms[i], terms[i + 1]) if i + 1 < len(terms) else terms[i]
                for i in range(0, len(terms), 2)
            ]
        part = terms[0][0] * (1.0 / terms[0][1])
        total = part if total is None else total + part
    return total


def halves(value):
    high = value.astype(jnp.bfloat16)
    return high, (value - high.astype(jnp.float32)).astype(jnp.bfloat16)


def outer_halves(value):
    high = lax.reduce_precision(value, 8, 7)
    low = lax.reduce_precision(value - high, 8, 7)
    return high.astype(jnp.bfloat16), low.astype(jnp.bfloat16)


def dot3(a_high, a_low, b_high, b_low):
    dot = functools.partial(jnp.dot, preferred_element_type=jnp.float32)
    return dot(a_high, b_high) + (dot(a_high, b_low) + dot(a_low, b_high))


def share_kernel(span_x, span_y, mine, out, send_sem, recv_sem, own_sem):
    devices = span_x * span_y
    gx, gy = lax.axis_index("gx"), lax.axis_index("gy")
    me = gx * span_y + gy

    def each_peer(act):
        def body(n, carry):
            i = lax.rem(gx + n // span_y, span_x)
            j = lax.rem(gy + n % span_y, span_y)
            act({"gx": i, "gy": j})
            return carry

        lax.fori_loop(1, devices, body, 0)

    barrier = pltpu.get_barrier_semaphore()
    each_peer(lambda peer: pl.semaphore_signal(barrier, inc=1, device_id=peer, device_id_type=MESH))
    own = pltpu.make_async_copy(mine, out.at[me], own_sem)
    own.start()
    pl.semaphore_wait(barrier, devices - 1)

    def send(peer):
        pltpu.make_async_remote_copy(
            src_ref=mine,
            dst_ref=out.at[me],
            send_sem=send_sem,
            recv_sem=recv_sem,
            device_id=peer,
            device_id_type=MESH,
        ).start()

    each_peer(send)
    own.wait()
    some = out.at[pl.ds(0, devices - 1)]
    pltpu.make_async_copy(some, some, send_sem).wait()
    pltpu.make_async_copy(some, some, recv_sem).wait()


def share(mine, span_x, span_y):
    inside = pl.BlockSpec(memory_space=pltpu.VMEM)
    return pl.pallas_call(
        functools.partial(share_kernel, span_x, span_y),
        in_specs=[inside],
        out_specs=inside,
        out_shape=jax.ShapeDtypeStruct((span_x * span_y,) + mine.shape, mine.dtype),
        scratch_shapes=[pltpu.SemaphoreType.DMA] * 3,
        compiler_params=pltpu.CompilerParams(collective_id=1, has_side_effects=True),
        name="share",
    )(mine)


def exchange_kernel(
    span_x, span_y, growth, capacity, log_crit, bins_ref, live_ref, route_ref, table_ref, rise_ref,
    source_ref, place_ref, cy_high, cy_low, cx_high, cx_low,
    recomb, out, load_ref,
    field, buf, coef_a, coef_b, sums, loads, load_parts, own, line, packed, arrived, stage,
    high, low, field_sems, recomb_sem,
    first_send, first_recv, first_own, line_send, line_recv, far_send, far_recv,
    back_send, back_recv, back_own, load_sems,
):
    steps, group, cells_y, cells_x = buf.shape
    depth_all = steps * group
    size_y, size_x = high.shape
    tiles = source_ref.shape[1]
    edge = depth_all // tiles
    per_tile = steps // tiles
    pairs = len(growth)
    bins_total = table_ref.shape[1]
    part = group // span_x
    rows = part * cells_y
    per = 128 // edge
    packs = packed.shape[1]
    lane_blocks = size_x // 128
    block = 128
    gx, gy = lax.axis_index("gx"), lax.axis_index("gy")
    level, w = gy // part, lax.rem(gy, part)
    half, side = level // 2, lax.rem(level, 2)
    mate = 2 * half + 1 - side
    me = gx * part + w
    is_middle = (level == 1) | (level == 2)
    is_end = (level == 0) | (level == 3)

    def at(i, j):
        return {"gx": i, "gy": j}

    def place(ref, s, i, j):
        return ref.at[
            s,
            pl.ds(pl.multiple_of(j * cells_y, cells_y), cells_y),
            pl.ds(pl.multiple_of(i * cells_x, cells_x), cells_x),
        ]

    def each_of_level(act):
        def body(n, carry):
            act(lax.rem(gx + n // part, span_x), lax.rem(w + n % part, part))
            return carry

        lax.fori_loop(1, group, body, 0)

    def every_peer(act):
        def body(n, carry):
            act(lax.rem(gx + n // span_y, span_x), lax.rem(gy + n % span_y, span_y))
            return carry

        lax.fori_loop(1, span_x * span_y, body, 0)

    barrier = pltpu.get_barrier_semaphore()
    every_peer(
        lambda i, j: pl.semaphore_signal(barrier, inc=1, device_id=at(i, j), device_id_type=MESH)
    )
    fetches = field_sems.shape[0]
    fetch_rows = cells_y // fetches

    def fetch(n):
        part_rows = pl.ds(n * fetch_rows, fetch_rows)
        return pltpu.make_async_copy(
            log_crit.at[:, part_rows], field.at[:, part_rows], field_sems.at[n]
        )

    for n in range(fetches):
        fetch(n).start()

    def first(s):
        def act(i, j):
            pltpu.make_async_remote_copy(
                src_ref=buf.at[s, i * part + j],
                dst_ref=place(own, s, gx, w),
                send_sem=first_send.at[s],
                recv_sem=first_recv.at[s],
                device_id=at(i, level * part + j),
                device_id_type=MESH,
            ).start()

        each_of_level(act)
        pltpu.make_async_copy(buf.at[s, me], place(own, s, gx, w), first_own.at[s]).start()

    def send_back(s):
        def act(i, j):
            pltpu.make_async_remote_copy(
                src_ref=place(line, s, i, j),
                dst_ref=out.at[s, me],
                send_sem=back_send.at[s],
                recv_sem=back_recv.at[s],
                device_id=at(i, level * part + j),
                device_id_type=MESH,
            ).start()

        each_of_level(act)
        pltpu.make_async_copy(place(line, s, gx, w), out.at[s, me], back_own.at[s]).start()

    def to_mate(source, s):
        return pltpu.make_async_remote_copy(
            src_ref=source.at[s],
            dst_ref=line.at[s],
            send_sem=line_send.at[s],
            recv_sem=line_recv.at[s],
            device_id=at(gx, mate * part + w),
            device_id_type=MESH,
        )

    def to_far(s):
        return pltpu.make_async_remote_copy(
            src_ref=packed.at[s],
            dst_ref=arrived.at[s],
            send_sem=far_send.at[s],
            recv_sem=far_recv.at[s],
            device_id=at(gx, (3 - level) * part + w),
            device_id_type=MESH,
        )

    def wait_others(sem, s):
        some = buf.at[0, pl.ds(0, group - 1)]
        pltpu.make_async_copy(some, some, sem.at[s]).wait()

    def wait_own(sem, s):
        one = buf.at[0, 0]
        pltpu.make_async_copy(one, one, sem.at[s]).wait()

    def wait_plane(sem, s):
        pltpu.make_async_copy(own.at[s], own.at[s], sem.at[s]).wait()

    def wait_packed(sem, s):
        pltpu.make_async_copy(packed.at[s], packed.at[s], sem.at[s]).wait()

    def turn_in(t):
        span = slice(t * edge, (t + 1) * edge)

        def one(row, carry):
            turned = field[:, row, span].T
            buf[pl.ds(t * per_tile, per_tile), :, row, :] = turned.reshape(per_tile, group, cells_x)
            return carry

        lax.fori_loop(0, cells_y, one, 0, unroll=4)

    def gather(t):
        def one(row, carry):
            kinds = lax.broadcasted_iota(jnp.int32, (bins_total, cells_x), 0)
            onehot = jnp.where(kinds == bins_ref[t, pl.ds(row, 1), :], 1.0, 0.0)
            rates = jnp.dot(
                table_ref[...], onehot.astype(jnp.bfloat16), preferred_element_type=jnp.float32
            )
            rates = rates * live_ref[t, pl.ds(row // edge, 1), :]
            upper, lower = rates[:pairs], rates[pairs:]
            coef_a[:, row, :] = upper + lower
            coef_b[:, row, :] = upper * rise_ref[1] + lower * rise_ref[0]
            return carry

        lax.fori_loop(0, cells_y, one, 0, unroll=4)
        sums[t] = jnp.zeros(sums.shape[1:], jnp.float32)

    def evaluate(s):
        t = s // per_tile
        batch = 4

        def one(n, carry):
            rows = pl.ds(pl.multiple_of(n // (group // batch) * 8, 8), 8)
            planes = pl.ds(n % (group // batch) * batch, batch)
            value = integral(
                buf[s, planes, rows, :], growth,
                lambda p: coef_a[p, rows, :], lambda p: coef_b[p, rows, :],
            )
            buf[s, planes, rows, :] = value
            sums[t, rows, :] += jnp.sum(value, axis=0)
            return carry

        lax.fori_loop(0, cells_y // 8 * (group // batch), one, 0)

    def turn_out(start, count):
        def one(n, carry):
            row = start + n
            flat = buf[:, :, row, :].reshape(depth_all, cells_x)
            field[:, row, :] = flat.T
            return carry

        lax.fori_loop(0, count, one, 0, unroll=2)

    def send_loads():
        blocks_y = live_ref.shape[1]
        lines = [
            jnp.sum(sums[t, b * edge : (b + 1) * edge, :], axis=0, keepdims=True)
            for t in range(tiles)
            for b in range(blocks_y)
        ]
        for g in range(span_y):
            share_of = None
            for n, line_sum in enumerate(lines):
                chosen = jnp.where(route_ref[pl.ds(n, 1), :] == g, line_sum, 0.0)
                share_of = chosen if share_of is None else share_of + chosen
            total = jnp.sum(share_of, axis=1, keepdims=True) / (edge * edge * edge) / capacity
            loads[g] = jnp.broadcast_to(total, (8, 128))
        pltpu.make_async_copy(loads.at[gy], load_parts.at[gy], load_sems.at[2]).start()

        def send(n, carry):
            j = lax.rem(gy + n, span_y)
            pltpu.make_async_remote_copy(
                src_ref=loads.at[j],
                dst_ref=load_parts.at[gy],
                send_sem=load_sems.at[0],
                recv_sem=load_sems.at[1],
                device_id=at(gx, j),
                device_id_type=MESH,
            ).start()
            return carry

        lax.fori_loop(1, span_y, send, 0)

    lane = lax.broadcasted_iota(jnp.int32, (edge, 128), 1)

    def rows_at(start, count):
        return pl.ds(pl.multiple_of(start, count), count)

    def turns(value):
        return [value if r == 0 else pltpu.roll(value, r * edge, 1) for r in range(per)]

    def pack(s):
        def fill(n, carry):
            down, across = n // lane_blocks, pl.ds(pl.multiple_of(n % lane_blocks * 128, 128), 128)
            chunk = rows_at(down * edge, edge)
            strip = rows // edge * lane_blocks
            for r, value in enumerate(turns(own[s, chunk, across])):
                stage[(side * strip + n) * per + r] = value
            for r, value in enumerate(turns(line[s, chunk, across])):
                stage[((1 - side) * strip + n) * per + r] = value
            return carry

        lax.fori_loop(0, rows // edge * lane_blocks, fill, 0)
        t = s // per_tile

        def one(g, carry):
            total = None
            for q in range(per):
                piece = stage[source_ref[half, t, g * per + q]]
                total = piece if total is None else jnp.where(lane >= q * edge, piece, total)
            packed[s, g] = total
            return carry

        lax.fori_loop(0, packs, one, 0)

    def unpack(s):
        for r in range(per):
            stage[r] = jnp.zeros((edge, 128), jnp.float32)
        def fill(g, carry):
            for r, value in enumerate(turns(arrived[s, g])):
                stage[(g + 1) * per + r] = value
            return carry

        lax.fori_loop(0, packs, fill, 0)
        t = s // per_tile

        def one(n, carry):
            down, block_x = n // lane_blocks, lax.rem(n, lane_blocks)
            total = None
            for q in range(per):
                piece = stage[place_ref[1 - half, t, n * per + q]]
                total = piece if total is None else jnp.where(lane >= q * edge, piece, total)
            to = (
                rows_at((1 - half) * 2 * rows + down * edge, edge),
                rows_at(block_x * 128, 128),
            )
            high[to], low[to] = halves(total)
            return carry

        lax.fori_loop(0, 2 * rows // edge * lane_blocks, one, 0)

    def split(source, s, which):
        def one(r, carry):
            to = rows_at(which * rows + r * block, block)
            high[to, :], low[to, :] = halves(source[s, rows_at(r * block, block), :])
            return carry

        lax.fori_loop(0, rows // block, one, 0)

    def along_y(which, r):
        chunk = rows_at(which * rows + r * block, block)
        return dot3(cy_high[chunk, :], cy_low[chunk, :], high[...], low[...])

    def along_x(value):
        return dot3(*halves(value), cx_high[...], cx_low[...])

    def middle_first(s):
        wait_own(first_own, s)
        wait_others(first_recv, s)
        wait_plane(line_recv, s)
        pack(s)
        to_far(s).start()

    def middle_second(s):
        split(own, s, level)
        split(line, s, mate)
        wait_packed(far_recv, s)
        unpack(s)

        def for_mate(r, carry):
            own[s, rows_at(r * block, block), :] = along_y(mate, r)
            return carry

        lax.fori_loop(0, rows // block, for_mate, 0)
        to_mate(own, s).start()

        def for_me(r, carry):
            line[s, rows_at(r * block, block), :] = along_x(along_y(level, r))
            return carry

        lax.fori_loop(0, rows // block, for_me, 0)
        send_back(s)

    def end_first(s):
        wait_own(first_own, s)
        wait_others(first_recv, s)
        to_mate(own, s).start()

    def end_second(s):
        wait_plane(line_recv, s)

        def for_me(r, carry):
            line[s, rows_at(r * block, block), :] = along_x(line[s, rows_at(r * block, block), :])
            return carry

        lax.fori_loop(0, rows // block, for_me, 0)
        send_back(s)

    last = 6
    out_rounds = 4

    def at_step(i, who, lag, act):
        @pl.when(who & (i >= lag) & (i < steps + lag))
        def _():
            act(i - lag)

    def body(i, carry):
        for t in range(tiles):
            @pl.when(i == t * per_tile)
            def _():
                if t == 0:
                    for n in range(fetches):
                        fetch(n).wait()
                turn_in(t)
                gather(t)

        @pl.when(i < steps)
        def _():
            evaluate(i)

        @pl.when(i == 0)
        def _():
            pl.semaphore_wait(barrier, span_x * span_y - 1)

        @pl.when(i < steps)
        def _():
            first(i)

        at_step(i, is_end, 1, end_first)
        at_step(i, is_middle, 2, middle_first)
        at_step(i, is_middle, 4, middle_second)
        at_step(i, is_end, last, end_second)

        @pl.when(i == steps)
        def _():
            send_loads()

        @pl.when((i >= steps) & (i < steps + out_rounds))
        def _():
            turn_out((i - steps) * (cells_y // out_rounds), cells_y // out_rounds)

        return carry

    lax.fori_loop(0, steps + last, body, 0)
    write = pltpu.make_async_copy(field, recomb, recomb_sem)
    write.start()

    @pl.when(is_middle)
    def _():
        def drain(s, carry):
            wait_packed(far_send, s)
            return carry

        lax.fori_loop(0, steps, drain, 0)

    some_loads = loads.at[pl.ds(0, span_y - 1)]
    pltpu.make_async_copy(some_loads, some_loads, load_sems.at[0]).wait()
    pltpu.make_async_copy(some_loads, some_loads, load_sems.at[1]).wait()
    pltpu.make_async_copy(loads.at[0], loads.at[0], load_sems.at[2]).wait()
    load_ref[...] = jnp.sum(load_parts[...], axis=0)

    def finish(s, carry):
        wait_plane(line_send, s)
        wait_others(first_send, s)
        wait_others(back_send, s)
        wait_own(back_own, s)
        wait_others(back_recv, s)
        return carry

    lax.fori_loop(0, steps, finish, 0)
    write.wait()


def exchange(
    slots, collective, span_x, span_y, growth, capacity, log_crit, bins, live, routes, table, rise,
    source, position, cy_high, cy_low, cx_high, cx_low,
):
    cells_x, cells_y, depth_all = log_crit.shape
    group = span_x * span_y // levels
    steps = depth_all // group
    edge = depth_all // source.shape[1]
    size_y, size_x = cy_high.shape[0], cx_high.shape[0]
    rows = size_y // levels
    packs = slots * edge // 128
    per = 128 // edge
    stage_size = max(2 * rows * size_x // edge // edge, per * (packs + 1))
    anywhere = pl.BlockSpec(memory_space=pl.ANY)
    inside = pl.BlockSpec(memory_space=pltpu.VMEM)
    scalars = pl.BlockSpec(memory_space=pltpu.SMEM)
    planes = pltpu.VMEM((steps, rows, size_x), jnp.float32)
    packing = pltpu.VMEM((steps, packs, edge, 128), jnp.float32)
    coefs = pltpu.VMEM((len(growth), cells_y, cells_x), jnp.float32)
    parts = pltpu.VMEM((span_y, 8, 128), jnp.float32)
    halved = pltpu.VMEM((size_y, size_x), jnp.bfloat16)
    sems = pltpu.SemaphoreType.DMA((steps,))
    return pl.pallas_call(
        functools.partial(exchange_kernel, span_x, span_y, growth, capacity),
        in_specs=[anywhere] + [inside] * 5 + [scalars] * 2 + [inside] * 4,
        out_specs=[anywhere] * 2 + [inside],
        out_shape=[
            jax.ShapeDtypeStruct(log_crit.shape, jnp.float32),
            jax.ShapeDtypeStruct((steps, group, cells_y, cells_x), jnp.float32),
            jax.ShapeDtypeStruct((8, 128), jnp.float32),
        ],
        scratch_shapes=[
            pltpu.VMEM(log_crit.shape, jnp.float32),
            pltpu.VMEM((steps, group, cells_y, cells_x), jnp.float32),
            coefs,
            coefs,
            pltpu.VMEM((source.shape[1], cells_y, cells_x), jnp.float32),
            parts,
            parts,
            planes,
            planes,
            packing,
            packing,
            pltpu.VMEM((stage_size, edge, 128), jnp.float32),
            halved,
            halved,
            pltpu.SemaphoreType.DMA((4,)),
            pltpu.SemaphoreType.DMA,
        ]
        + [sems] * 10
        + [pltpu.SemaphoreType.DMA((3,))],
        compiler_params=pltpu.CompilerParams(
            collective_id=collective, has_side_effects=True, vmem_limit_bytes=vmem_grant
        ),
        name=f"exchange{slots}",
    )(
        log_crit, bins, live, routes, table, rise, source, position, cy_high, cy_low, cx_high,
        cx_low,
    )


def slot_tables(masks, edge):
    halves_count = 2
    flat = masks.reshape(halves_count, -1, masks.shape[2]).transpose(0, 2, 1)
    slots = flat.shape[2]
    before = jnp.triu(jnp.ones((slots, slots), jnp.bfloat16), 1)
    rank = jnp.dot(flat.astype(jnp.bfloat16), before, preferred_element_type=jnp.float32)
    rank = rank.astype(jnp.int32)
    per = 128 // edge
    indices = jnp.arange(slots, dtype=jnp.int32)
    shifted = (indices % per - rank) % per
    position = jnp.where(flat == 1, rank, -1)
    place = jnp.where(flat == 1, (rank // per + 1) * per + shifted, 0)
    from_place = indices // per * per + (rank - indices) % per
    source = jnp.sum(
        jnp.where(position[:, :, None, :] == indices[:, None], from_place[:, :, None, :], 0), axis=3
    )
    most = jnp.max(jnp.sum(flat, axis=2))
    return source, place, most


def turn_kernel(source_ref, out_ref):
    for row in range(source_ref.shape[1]):
        out_ref[:, row, :] = source_ref[:, row, :].T


def turn(source):
    depth_all, cells_y, cells_x = source.shape
    rows = 8
    return pl.pallas_call(
        turn_kernel,
        grid=(cells_y // rows,),
        in_specs=[pl.BlockSpec((depth_all, rows, cells_x), lambda j: (0, j, 0))],
        out_specs=pl.BlockSpec((cells_x, rows, depth_all), lambda j: (0, j, 0)),
        out_shape=jax.ShapeDtypeStruct((cells_x, cells_y, depth_all), jnp.float32),
        name="turn",
    )(source)


def wave_freq(length):
    half = length // 2
    return jnp.concatenate(
        [jnp.arange(half + 1, dtype=jnp.int32), jnp.arange(1, half, dtype=jnp.int32)]
    )


def wave_table(length):
    half = length // 2
    indices = jnp.arange(length, dtype=jnp.int32)
    turns = indices[:, None] * wave_freq(length)[None, :] % length
    angles = 2.0 * math.pi / length * turns.astype(jnp.float32)
    shift = jnp.where(indices < half + 1, 0.0, math.pi / 2)[None, :]
    return lax.optimization_barrier(jnp.cos(angles - shift))


def circulant(gain, table):
    length = gain.shape[0]
    half = length // 2
    freq = wave_freq(length)
    weight = jnp.concatenate([gain[: half + 1], gain[1:half]])
    doubled = jnp.where((freq == 0) | (freq == half), 1.0, 2.0).astype(jnp.float32)
    scaled = lax.optimization_barrier(table * (weight * doubled / length))
    return lax.dot_general(
        scaled, table, (((1,), (1,)), ((), ())), precision=lax.Precision.HIGHEST
    )


def on_device(log_crit, col_bins, rate_table, tile_mask, tile_route, filt_x, filt_y):
    blocks_x, blocks_y, tiles = tile_mask.shape
    cells_x, cells_y, depth_all = log_crit.shape
    edge = cells_x // blocks_x
    span_x, span_y = lax.axis_size("gx"), lax.axis_size("gy")
    devices = span_x * span_y
    nodes = rate_table.shape[1]
    half = nodes // 2

    bins = col_bins.transpose(2, 1, 0)
    live = jnp.repeat((tile_mask == 1).astype(jnp.float32).transpose(2, 1, 0), edge, axis=2)
    routes = jnp.repeat(
        tile_route.transpose(2, 1, 0).reshape(tiles * blocks_y, blocks_x), edge, axis=1
    )
    table = jnp.concatenate([rate_table[:, half:], rate_table[:, half - 1 :: -1]], axis=1).T

    growth = node_growth(nodes)
    ends = np.array([growth, [1.0 / e for e in growth]], np.float32)
    rise = jnp.asarray(np.broadcast_to(ends[:, :, None], (2, half, cells_x)))
    capacity = blocks_x * blocks_y * tiles // 2
    table_x = wave_table(filt_x.shape[0])
    table_y = table_x if filt_y.shape == filt_x.shape else wave_table(filt_y.shape[0])
    mine = jnp.pad((tile_mask == 1).astype(jnp.int32).reshape(1, -1), ((0, 7), (0, 128 - blocks_x * blocks_y * tiles)))
    masks = share(mine, span_x, span_y)[:, 0, : blocks_x * blocks_y * tiles]
    masks = masks.reshape(span_x, span_y, blocks_x, blocks_y, tiles).transpose(1, 3, 0, 2, 4)
    masks = masks.reshape(span_y * blocks_y, span_x * blocks_x, tiles)
    source, position, most = slot_tables(masks, edge)
    every = position.shape[2]
    few = every * 19 // 32
    operands = (
        log_crit, bins, live, routes, table, rise, source, position,
        *outer_halves(circulant(filt_y, table_y)), *outer_halves(circulant(filt_x, table_x)),
    )

    def run(slots, collective):
        return lambda *args: exchange(slots, collective, span_x, span_y, growth, capacity, *args)

    recomb, back, device_load = lax.cond(most <= few, run(few, 2), run(every, 3), *operands)
    smoothed = turn(back.reshape(depth_all, cells_y, cells_x))
    return (recomb, smoothed, device_load[:1, :1])


def solution(mesh):
    placed = (
        P("gx", "gy", None),
        P("gx", "gy", None),
        P(),
        P("gx", "gy", None),
        P("gx", "gy", None),
        P(),
        P(),
    )
    return jax.shard_map(
        on_device,
        mesh=mesh,
        in_specs=placed,
        out_specs=(P("gx", "gy", None), P("gx", "gy", None), P("gx", "gy")),
        check_vma=False,
    )
```

```python
import functools
import math

import jax
import jax.numpy as jnp
import numpy as np
from jax import lax
from jax.experimental import pallas as pl
from jax.experimental.pallas import tpu as pltpu
from jax.sharding import PartitionSpec as P

steepness = 3.0
vmem_grant = 60 * 1024 * 1024
MESH = pl.DeviceIdType.MESH
levels = 4


def node_growth(nodes):
    return [math.exp(steepness * (-2.5 + 5.0 * q / (nodes - 1))) for q in range(nodes // 2, nodes)]


def join(left, right):
    num_left, den_left = left
    num_right, den_right = right
    return (num_left * den_right + num_right * den_left, den_left * den_right)


def integral(field, growth, coef_a, coef_b):
    pairs = len(growth)
    v = jnp.exp(field * steepness)
    y = v + jnp.exp(field * -steepness)
    total = None
    for first in range(0, pairs, 4):
        terms = []
        for p in range(first, min(first + 4, pairs)):
            num = coef_a(p) * v + coef_b(p)
            terms.append((num, y + (growth[p] + 1.0 / growth[p])))
        while len(terms) > 1:
            terms = [
                join(terms[i], terms[i + 1]) if i + 1 < len(terms) else terms[i]
                for i in range(0, len(terms), 2)
            ]
        part = terms[0][0] * (1.0 / terms[0][1])
        total = part if total is None else total + part
    return total


def halves(value):
    high = value.astype(jnp.bfloat16)
    return high, (value - high.astype(jnp.float32)).astype(jnp.bfloat16)


def outer_halves(value):
    high = lax.reduce_precision(value, 8, 7)
    low = lax.reduce_precision(value - high, 8, 7)
    return high.astype(jnp.bfloat16), low.astype(jnp.bfloat16)


def dot3(a_high, a_low, b_high, b_low):
    dot = functools.partial(jnp.dot, preferred_element_type=jnp.float32)
    return dot(a_high, b_high) + (dot(a_high, b_low) + dot(a_low, b_high))


def share_kernel(span_x, span_y, mine, out, send_sem, recv_sem, own_sem):
    devices = span_x * span_y
    gx, gy = lax.axis_index("gx"), lax.axis_index("gy")
    me = gx * span_y + gy

    def each_peer(act):
        def body(n, carry):
            i = lax.rem(gx + n // span_y, span_x)
            j = lax.rem(gy + n % span_y, span_y)
            act({"gx": i, "gy": j})
            return carry

        lax.fori_loop(1, devices, body, 0)

    barrier = pltpu.get_barrier_semaphore()
    each_peer(lambda peer: pl.semaphore_signal(barrier, inc=1, device_id=peer, device_id_type=MESH))
    own = pltpu.make_async_copy(mine, out.at[me], own_sem)
    own.start()
    pl.semaphore_wait(barrier, devices - 1)

    def send(peer):
        pltpu.make_async_remote_copy(
            src_ref=mine,
            dst_ref=out.at[me],
            send_sem=send_sem,
            recv_sem=recv_sem,
            device_id=peer,
            device_id_type=MESH,
        ).start()

    each_peer(send)
    own.wait()
    some = out.at[pl.ds(0, devices - 1)]
    pltpu.make_async_copy(some, some, send_sem).wait()
    pltpu.make_async_copy(some, some, recv_sem).wait()


def share(mine, span_x, span_y):
    inside = pl.BlockSpec(memory_space=pltpu.VMEM)
    return pl.pallas_call(
        functools.partial(share_kernel, span_x, span_y),
        in_specs=[inside],
        out_specs=inside,
        out_shape=jax.ShapeDtypeStruct((span_x * span_y,) + mine.shape, mine.dtype),
        scratch_shapes=[pltpu.SemaphoreType.DMA] * 3,
        compiler_params=pltpu.CompilerParams(collective_id=1, has_side_effects=True),
        name="share",
    )(mine)


def exchange_kernel(
    span_x, span_y, growth, capacity, log_crit, bins_ref, live_ref, route_ref, table_ref, rise_ref,
    source_ref, place_ref, cy_high, cy_low, cx_high, cx_low,
    recomb, out, load_ref,
    field, buf, known, coefs, sums, loads, load_parts, own, line, packed, arrived, stage,
    high, low, field_sems, recomb_sem,
    first_send, first_recv, first_own, line_send, line_recv, far_send, far_recv,
    back_send, back_recv, back_own, load_sems,
):
    steps, group, cells_y, cells_x = buf.shape
    depth_all = steps * group
    size_y, size_x = high.shape
    tiles = source_ref.shape[1]
    edge = depth_all // tiles
    per_tile = steps // tiles
    pairs = len(growth)
    part = group // span_x
    rows = part * cells_y
    per = 128 // edge
    packs = packed.shape[1]
    lane_blocks = size_x // 128
    block = 128
    gx, gy = lax.axis_index("gx"), lax.axis_index("gy")
    level, w = gy // part, lax.rem(gy, part)
    half, side = level // 2, lax.rem(level, 2)
    mate = 2 * half + 1 - side
    me = gx * part + w
    is_middle = (level == 1) | (level == 2)
    is_end = (level == 0) | (level == 3)

    def at(i, j):
        return {"gx": i, "gy": j}

    def place(ref, s, i, j):
        return ref.at[
            s,
            pl.ds(pl.multiple_of(j * cells_y, cells_y), cells_y),
            pl.ds(pl.multiple_of(i * cells_x, cells_x), cells_x),
        ]

    def each_of_level(act):
        def body(n, carry):
            act(lax.rem(gx + n // part, span_x), lax.rem(w + n % part, part))
            return carry

        lax.fori_loop(1, group, body, 0)

    def every_peer(act):
        def body(n, carry):
            act(lax.rem(gx + n // span_y, span_x), lax.rem(gy + n % span_y, span_y))
            return carry

        lax.fori_loop(1, span_x * span_y, body, 0)

    barrier = pltpu.get_barrier_semaphore()
    every_peer(
        lambda i, j: pl.semaphore_signal(barrier, inc=1, device_id=at(i, j), device_id_type=MESH)
    )
    fetches = field_sems.shape[0]
    fetch_rows = cells_y // fetches

    def fetch(n):
        part_rows = pl.ds(n * fetch_rows, fetch_rows)
        return pltpu.make_async_copy(
            log_crit.at[:, part_rows], field.at[:, part_rows], field_sems.at[n]
        )

    for n in range(fetches):
        fetch(n).start()

    def first(s):
        def act(i, j):
            pltpu.make_async_remote_copy(
                src_ref=buf.at[s, i * part + j],
                dst_ref=place(own, s, gx, w),
                send_sem=first_send.at[s],
                recv_sem=first_recv.at[s],
                device_id=at(i, level * part + j),
                device_id_type=MESH,
            ).start()

        each_of_level(act)
        pltpu.make_async_copy(buf.at[s, me], place(own, s, gx, w), first_own.at[s]).start()

    def send_back(s):
        def act(i, j):
            pltpu.make_async_remote_copy(
                src_ref=place(line, s, i, j),
                dst_ref=out.at[s, me],
                send_sem=back_send.at[s],
                recv_sem=back_recv.at[s],
                device_id=at(i, level * part + j),
                device_id_type=MESH,
            ).start()

        each_of_level(act)
        pltpu.make_async_copy(place(line, s, gx, w), out.at[s, me], back_own.at[s]).start()

    def to_mate(source, s):
        return pltpu.make_async_remote_copy(
            src_ref=source.at[s],
            dst_ref=line.at[s],
            send_sem=line_send.at[s],
            recv_sem=line_recv.at[s],
            device_id=at(gx, mate * part + w),
            device_id_type=MESH,
        )

    def to_far(s):
        return pltpu.make_async_remote_copy(
            src_ref=packed.at[s],
            dst_ref=arrived.at[s],
            send_sem=far_send.at[s],
            recv_sem=far_recv.at[s],
            device_id=at(gx, (3 - level) * part + w),
            device_id_type=MESH,
        )

    def wait_others(sem, s):
        some = buf.at[0, pl.ds(0, group - 1)]
        pltpu.make_async_copy(some, some, sem.at[s]).wait()

    def wait_own(sem, s):
        one = buf.at[0, 0]
        pltpu.make_async_copy(one, one, sem.at[s]).wait()

    def wait_plane(sem, s):
        pltpu.make_async_copy(own.at[s], own.at[s], sem.at[s]).wait()

    def wait_packed(sem, s):
        pltpu.make_async_copy(packed.at[s], packed.at[s], sem.at[s]).wait()

    def unrolled(count, width, act):
        def some(n, carry):
            for r in range(width):
                act(n * width + r)
            return carry

        lax.fori_loop(0, count // width, some, 0)
        for n in range(count // width * width, count):
            act(n)

    def turned(value):
        flat = jnp.swapaxes(value, 0, 1)
        return jnp.swapaxes(jnp.stack([flat[r].T for r in range(8)]), 0, 1)

    def eight(n):
        return pl.ds(pl.multiple_of(n * 8, 8), 8)

    def turn_in():
        def one(n, carry):
            value = turned(field[:, eight(n), :])
            buf[:, :, eight(n), :] = value.reshape(steps, group, 8, cells_x)
            return carry

        lax.fori_loop(0, cells_y // 8, one, 0)

    def turn_out(n):
        value = buf[:, :, eight(n), :].reshape(depth_all, 8, cells_x)
        field[:, eight(n), :] = turned(value)

    def tabulate():
        rates = table_ref[...].astype(jnp.float32)
        upper, lower = rates[:pairs], rates[pairs:]
        known[:pairs] = upper + lower
        known[pairs:] = upper * rise_ref[1] + lower * rise_ref[0]

    def gather(t):
        def one(n, carry):
            kinds = bins_ref[t, eight(n), :]
            live = jnp.broadcast_to(live_ref[t, pl.ds(n * 8 // edge, 1), :], kinds.shape)
            for p in range(2 * pairs):
                row = jnp.broadcast_to(known[pl.ds(p, 1), :], kinds.shape)
                coefs[p, eight(n), :] = live * jnp.take_along_axis(
                    row, kinds, axis=1, mode="promise_in_bounds"
                )
            return carry

        lax.fori_loop(0, cells_y // 8, one, 0)
        sums[t] = jnp.zeros(sums.shape[1:], jnp.float32)

    def evaluate(s):
        t = s // per_tile
        batch = 4

        def one(n, carry):
            rows = pl.ds(pl.multiple_of(n // (group // batch) * 8, 8), 8)
            planes = pl.ds(n % (group // batch) * batch, batch)
            value = integral(
                buf[s, planes, rows, :], growth,
                lambda p: coefs[p, rows, :], lambda p: coefs[pairs + p, rows, :],
            )
            buf[s, planes, rows, :] = value
            sums[t, rows, :] += jnp.sum(value, axis=0)
            return carry

        lax.fori_loop(0, cells_y // 8 * (group // batch), one, 0)

    def send_loads():
        blocks_y = live_ref.shape[1]
        lines = [
            jnp.sum(sums[t, b * edge : (b + 1) * edge, :], axis=0, keepdims=True)
            for t in range(tiles)
            for b in range(blocks_y)
        ]
        for g in range(span_y):
            share_of = None
            for n, line_sum in enumerate(lines):
                chosen = jnp.where(route_ref[pl.ds(n, 1), :] == g, line_sum, 0.0)
                share_of = chosen if share_of is None else share_of + chosen
            total = jnp.sum(share_of, axis=1, keepdims=True) / (edge * edge * edge) / capacity
            loads[g] = jnp.broadcast_to(total, (8, 128))
        pltpu.make_async_copy(loads.at[gy], load_parts.at[gy], load_sems.at[2]).start()

        def send(n, carry):
            j = lax.rem(gy + n, span_y)
            pltpu.make_async_remote_copy(
                src_ref=loads.at[j],
                dst_ref=load_parts.at[gy],
                send_sem=load_sems.at[0],
                recv_sem=load_sems.at[1],
                device_id=at(gx, j),
                device_id_type=MESH,
            ).start()
            return carry

        lax.fori_loop(1, span_y, send, 0)

    lane = lax.broadcasted_iota(jnp.int32, (edge, 128), 1)

    def rows_at(start, count):
        return pl.ds(pl.multiple_of(start, count), count)

    def turns(value):
        return [value if r == 0 else pltpu.roll(value, r * edge, 1) for r in range(per)]

    def pack(s):
        strip = rows // edge * lane_blocks

        def fill(n):
            across = pl.ds(pl.multiple_of(n % lane_blocks * 128, 128), 128)
            chunk = rows_at(n // lane_blocks * edge, edge)
            for r, value in enumerate(turns(own[s, chunk, across])):
                stage[(side * strip + n) * per + r] = value
            for r, value in enumerate(turns(line[s, chunk, across])):
                stage[((1 - side) * strip + n) * per + r] = value

        unrolled(strip, 2, fill)
        t = s // per_tile

        def one(g):
            total = None
            for q in range(per):
                piece = stage[source_ref[half, t, g * per + q]]
                total = piece if total is None else jnp.where(lane >= q * edge, piece, total)
            packed[s, g] = total

        unrolled(packs, 4, one)

    def unpack(s):
        for r in range(per):
            stage[r] = jnp.zeros((edge, 128), jnp.float32)

        def fill(g):
            for r, value in enumerate(turns(arrived[s, g])):
                stage[(g + 1) * per + r] = value

        unrolled(packs, 4, fill)
        t = s // per_tile

        def one(n):
            down, block_x = n // lane_blocks, lax.rem(n, lane_blocks)
            total = None
            for q in range(per):
                piece = stage[place_ref[1 - half, t, n * per + q]]
                total = piece if total is None else jnp.where(lane >= q * edge, piece, total)
            to = (
                rows_at((1 - half) * 2 * rows + down * edge, edge),
                rows_at(block_x * 128, 128),
            )
            high[to], low[to] = halves(total)

        unrolled(2 * rows // edge * lane_blocks, 4, one)

    def split(source, s, which):
        def one(r, carry):
            to = rows_at(which * rows + r * block, block)
            high[to, :], low[to, :] = halves(source[s, rows_at(r * block, block), :])
            return carry

        lax.fori_loop(0, rows // block, one, 0)

    def along_y(which, r):
        chunk = rows_at(which * rows + r * block, block)
        return dot3(cy_high[chunk, :], cy_low[chunk, :], high[...], low[...])

    def along_x(value):
        return dot3(*halves(value), cx_high[...], cx_low[...])

    def middle_first(s):
        wait_own(first_own, s)
        wait_others(first_recv, s)
        wait_plane(line_recv, s)
        pack(s)
        to_far(s).start()

    def middle_second(s):
        split(own, s, level)
        split(line, s, mate)
        wait_packed(far_recv, s)
        unpack(s)

        def for_mate(r, carry):
            own[s, rows_at(r * block, block), :] = along_y(mate, r)
            return carry

        lax.fori_loop(0, rows // block, for_mate, 0)
        to_mate(own, s).start()

        def for_me(r, carry):
            line[s, rows_at(r * block, block), :] = along_x(along_y(level, r))
            return carry

        lax.fori_loop(0, rows // block, for_me, 0)
        send_back(s)

    def end_first(s):
        wait_own(first_own, s)
        wait_others(first_recv, s)
        to_mate(own, s).start()

    def end_second(s):
        wait_plane(line_recv, s)

        def for_me(r, carry):
            line[s, rows_at(r * block, block), :] = along_x(line[s, rows_at(r * block, block), :])
            return carry

        lax.fori_loop(0, rows // block, for_me, 0)
        send_back(s)

    lags = (1, 2, 4, 6)
    out_rounds = 4

    def at_step(i, who, lag, act):
        @pl.when(who & (i >= lag) & (i < steps + lag))
        def _():
            act(i - lag)

    def body(i, carry):
        at_step(i, is_end, lags[0], end_first)

        @pl.when((i < steps) & (i % per_tile == 0))
        def _():
            gather(i // per_tile)

        @pl.when(i < steps)
        def _():
            evaluate(i)

        @pl.when(i < steps)
        def _():
            first(i)

        at_step(i, is_middle, lags[1], middle_first)
        at_step(i, is_middle, lags[2], middle_second)
        at_step(i, is_end, lags[3], end_second)

        @pl.when(i == steps)
        def _():
            send_loads()

        @pl.when((i >= steps) & (i < steps + out_rounds))
        def _():
            for n in range(cells_y // 8 // out_rounds):
                turn_out((i - steps) * (cells_y // 8 // out_rounds) + n)

        return carry

    last = max(lags[3], out_rounds)
    tabulate()
    for n in range(fetches):
        fetch(n).wait()
    turn_in()
    pl.semaphore_wait(barrier, span_x * span_y - 1)
    lax.fori_loop(0, steps + last, body, 0)
    write = pltpu.make_async_copy(field, recomb, recomb_sem)
    write.start()

    @pl.when(is_middle)
    def _():
        def drain(s, carry):
            wait_packed(far_send, s)
            return carry

        lax.fori_loop(0, steps, drain, 0)

    some_loads = loads.at[pl.ds(0, span_y - 1)]
    pltpu.make_async_copy(some_loads, some_loads, load_sems.at[0]).wait()
    pltpu.make_async_copy(some_loads, some_loads, load_sems.at[1]).wait()
    pltpu.make_async_copy(loads.at[0], loads.at[0], load_sems.at[2]).wait()
    load_ref[...] = jnp.sum(load_parts[...], axis=0)

    def finish(s, carry):
        wait_plane(line_send, s)
        wait_others(first_send, s)
        wait_others(back_send, s)
        wait_own(back_own, s)
        wait_others(back_recv, s)
        return carry

    lax.fori_loop(0, steps, finish, 0)
    write.wait()


def exchange(
    slots, collective, span_x, span_y, growth, capacity, log_crit, bins, live, routes, table, rise,
    source, position, cy_high, cy_low, cx_high, cx_low,
):
    cells_x, cells_y, depth_all = log_crit.shape
    group = span_x * span_y // levels
    steps = depth_all // group
    edge = depth_all // source.shape[1]
    size_y, size_x = cy_high.shape[0], cx_high.shape[0]
    rows = size_y // levels
    packs = slots * edge // 128
    per = 128 // edge
    stage_size = max(2 * rows * size_x // edge // edge, per * (packs + 1))
    anywhere = pl.BlockSpec(memory_space=pl.ANY)
    inside = pl.BlockSpec(memory_space=pltpu.VMEM)
    scalars = pl.BlockSpec(memory_space=pltpu.SMEM)
    planes = pltpu.VMEM((steps, rows, size_x), jnp.float32)
    packing = pltpu.VMEM((steps, packs, edge, 128), jnp.float32)
    parts = pltpu.VMEM((span_y, 8, 128), jnp.float32)
    halved = pltpu.VMEM((size_y, size_x), jnp.bfloat16)
    sems = pltpu.SemaphoreType.DMA((steps,))
    return pl.pallas_call(
        functools.partial(exchange_kernel, span_x, span_y, growth, capacity),
        in_specs=[anywhere] + [inside] * 5 + [scalars] * 2 + [inside] * 4,
        out_specs=[anywhere] * 2 + [inside],
        out_shape=[
            jax.ShapeDtypeStruct(log_crit.shape, jnp.float32),
            jax.ShapeDtypeStruct((steps, group, cells_y, cells_x), jnp.float32),
            jax.ShapeDtypeStruct((8, 128), jnp.float32),
        ],
        scratch_shapes=[
            pltpu.VMEM(log_crit.shape, jnp.float32),
            pltpu.VMEM((steps, group, cells_y, cells_x), jnp.float32),
            pltpu.VMEM(table.shape, jnp.float32),
            pltpu.VMEM((2 * len(growth), cells_y, cells_x), jnp.float32),
            pltpu.VMEM((source.shape[1], cells_y, cells_x), jnp.float32),
            parts,
            parts,
            planes,
            planes,
            packing,
            packing,
            pltpu.VMEM((stage_size, edge, 128), jnp.float32),
            halved,
            halved,
            pltpu.SemaphoreType.DMA((4,)),
            pltpu.SemaphoreType.DMA,
        ]
        + [sems] * 10
        + [pltpu.SemaphoreType.DMA((3,))],
        compiler_params=pltpu.CompilerParams(
            collective_id=collective, has_side_effects=True, vmem_limit_bytes=vmem_grant
        ),
        name=f"exchange{slots}",
    )(
        log_crit, bins, live, routes, table, rise, source, position, cy_high, cy_low, cx_high,
        cx_low,
    )


def slot_tables(masks, edge):
    halves_count = 2
    flat = masks.reshape(halves_count, -1, masks.shape[2]).transpose(0, 2, 1)
    slots = flat.shape[2]
    before = jnp.triu(jnp.ones((slots, slots), jnp.bfloat16), 1)
    rank = jnp.dot(flat.astype(jnp.bfloat16), before, preferred_element_type=jnp.float32)
    rank = rank.astype(jnp.int32)
    per = 128 // edge
    indices = jnp.arange(slots, dtype=jnp.int32)
    shifted = (indices % per - rank) % per
    position = jnp.where(flat == 1, rank, -1)
    place = jnp.where(flat == 1, (rank // per + 1) * per + shifted, 0)
    from_place = indices // per * per + (rank - indices) % per
    source = jnp.sum(
        jnp.where(position[:, :, None, :] == indices[:, None], from_place[:, :, None, :], 0), axis=3
    )
    most = jnp.max(jnp.sum(flat, axis=2))
    return source, place, most


def turn_kernel(source_ref, out_ref):
    for row in range(source_ref.shape[1]):
        out_ref[:, row, :] = source_ref[:, row, :].T


def turn(source):
    depth_all, cells_y, cells_x = source.shape
    rows = 8
    return pl.pallas_call(
        turn_kernel,
        grid=(cells_y // rows,),
        in_specs=[pl.BlockSpec((depth_all, rows, cells_x), lambda j: (0, j, 0))],
        out_specs=pl.BlockSpec((cells_x, rows, depth_all), lambda j: (0, j, 0)),
        out_shape=jax.ShapeDtypeStruct((cells_x, cells_y, depth_all), jnp.float32),
        name="turn",
    )(source)


def wave_freq(length):
    half = length // 2
    return jnp.concatenate(
        [jnp.arange(half + 1, dtype=jnp.int32), jnp.arange(1, half, dtype=jnp.int32)]
    )


def wave_table(length):
    half = length // 2
    indices = jnp.arange(length, dtype=jnp.int32)
    turns = indices[:, None] * wave_freq(length)[None, :] % length
    angles = 2.0 * math.pi / length * turns.astype(jnp.float32)
    shift = jnp.where(indices < half + 1, 0.0, math.pi / 2)[None, :]
    return lax.optimization_barrier(jnp.cos(angles - shift))


def circulant(gain, table):
    length = gain.shape[0]
    half = length // 2
    freq = wave_freq(length)
    weight = jnp.concatenate([gain[: half + 1], gain[1:half]])
    doubled = jnp.where((freq == 0) | (freq == half), 1.0, 2.0).astype(jnp.float32)
    scaled = lax.optimization_barrier(table * (weight * doubled / length))
    return lax.dot_general(
        scaled, table, (((1,), (1,)), ((), ())), precision=lax.Precision.HIGHEST
    )


def on_device(log_crit, col_bins, rate_table, tile_mask, tile_route, filt_x, filt_y):
    blocks_x, blocks_y, tiles = tile_mask.shape
    cells_x, cells_y, depth_all = log_crit.shape
    edge = cells_x // blocks_x
    span_x, span_y = lax.axis_size("gx"), lax.axis_size("gy")
    devices = span_x * span_y
    nodes = rate_table.shape[1]
    half = nodes // 2

    bins = col_bins.transpose(2, 1, 0)
    live = jnp.repeat((tile_mask == 1).astype(jnp.float32).transpose(2, 1, 0), edge, axis=2)
    routes = jnp.repeat(
        tile_route.transpose(2, 1, 0).reshape(tiles * blocks_y, blocks_x), edge, axis=1
    )
    table = jnp.concatenate([rate_table[:, half:], rate_table[:, half - 1 :: -1]], axis=1).T

    growth = node_growth(nodes)
    ends = np.array([growth, [1.0 / e for e in growth]], np.float32)
    rise = jnp.asarray(np.broadcast_to(ends[:, :, None], (2, half, table.shape[1])))
    capacity = blocks_x * blocks_y * tiles // 2
    table_x = wave_table(filt_x.shape[0])
    table_y = table_x if filt_y.shape == filt_x.shape else wave_table(filt_y.shape[0])
    mine = jnp.pad((tile_mask == 1).astype(jnp.int32).reshape(1, -1), ((0, 7), (0, 128 - blocks_x * blocks_y * tiles)))
    masks = share(mine, span_x, span_y)[:, 0, : blocks_x * blocks_y * tiles]
    masks = masks.reshape(span_x, span_y, blocks_x, blocks_y, tiles).transpose(1, 3, 0, 2, 4)
    masks = masks.reshape(span_y * blocks_y, span_x * blocks_x, tiles)
    source, position, most = slot_tables(masks, edge)
    every = position.shape[2]
    few = every * 19 // 32
    operands = (
        log_crit, bins, live, routes, table, rise, source, position,
        *outer_halves(circulant(filt_y, table_y)), *outer_halves(circulant(filt_x, table_x)),
    )

    def run(slots, collective):
        return lambda *args: exchange(slots, collective, span_x, span_y, growth, capacity, *args)

    recomb, back, device_load = lax.cond(most <= few, run(few, 2), run(every, 3), *operands)
    smoothed = turn(back.reshape(depth_all, cells_y, cells_x))
    return (recomb, smoothed, device_load[:1, :1])


def solution(mesh):
    placed = (
        P("gx", "gy", None),
        P("gx", "gy", None),
        P(),
        P("gx", "gy", None),
        P("gx", "gy", None),
        P(),
        P(),
    )
    return jax.shard_map(
        on_device,
        mesh=mesh,
        in_specs=placed,
        out_specs=(P("gx", "gy", None), P("gx", "gy", None), P("gx", "gy")),
        check_vma=False,
    )
```

```python
import functools
import math

import jax
import jax.numpy as jnp
import numpy as np
from jax import lax
from jax.experimental import pallas as pl
from jax.experimental.pallas import tpu as pltpu
from jax.sharding import PartitionSpec as P

steepness = 3.0
vmem_grant = 60 * 1024 * 1024
MESH = pl.DeviceIdType.MESH
levels = 4


def node_growth(nodes):
    return [math.exp(steepness * (-2.5 + 5.0 * q / (nodes - 1))) for q in range(nodes // 2, nodes)]


def join(left, right):
    num_left, den_left = left
    num_right, den_right = right
    return (num_left * den_right + num_right * den_left, den_left * den_right)


def integral(field, growth, coef_a, coef_b):
    pairs = len(growth)
    v = jnp.exp(field * steepness)
    y = v + jnp.exp(field * -steepness)
    total = None
    for first in range(0, pairs, 4):
        terms = []
        for p in range(first, min(first + 4, pairs)):
            num = coef_a(p) * v + coef_b(p)
            terms.append((num, y + (growth[p] + 1.0 / growth[p])))
        while len(terms) > 1:
            terms = [
                join(terms[i], terms[i + 1]) if i + 1 < len(terms) else terms[i]
                for i in range(0, len(terms), 2)
            ]
        part = terms[0][0] * (1.0 / terms[0][1])
        total = part if total is None else total + part
    return total


def halves(value):
    high = value.astype(jnp.bfloat16)
    return high, (value - high.astype(jnp.float32)).astype(jnp.bfloat16)


def outer_halves(value):
    high = lax.reduce_precision(value, 8, 7)
    low = lax.reduce_precision(value - high, 8, 7)
    return high.astype(jnp.bfloat16), low.astype(jnp.bfloat16)


def dot3(a_high, a_low, b_high, b_low):
    dot = functools.partial(jnp.dot, preferred_element_type=jnp.float32)
    return dot(a_high, b_high) + (dot(a_high, b_low) + dot(a_low, b_high))


def share_kernel(span_x, span_y, mine, out, send_sem, recv_sem, own_sem):
    devices = span_x * span_y
    gx, gy = lax.axis_index("gx"), lax.axis_index("gy")
    me = gx * span_y + gy

    def each_peer(act):
        def body(n, carry):
            i = lax.rem(gx + n // span_y, span_x)
            j = lax.rem(gy + n % span_y, span_y)
            act({"gx": i, "gy": j})
            return carry

        lax.fori_loop(1, devices, body, 0)

    barrier = pltpu.get_barrier_semaphore()
    each_peer(lambda peer: pl.semaphore_signal(barrier, inc=1, device_id=peer, device_id_type=MESH))
    own = pltpu.make_async_copy(mine, out.at[me], own_sem)
    own.start()
    pl.semaphore_wait(barrier, devices - 1)

    def send(peer):
        pltpu.make_async_remote_copy(
            src_ref=mine,
            dst_ref=out.at[me],
            send_sem=send_sem,
            recv_sem=recv_sem,
            device_id=peer,
            device_id_type=MESH,
        ).start()

    each_peer(send)
    own.wait()
    some = out.at[pl.ds(0, devices - 1)]
    pltpu.make_async_copy(some, some, send_sem).wait()
    pltpu.make_async_copy(some, some, recv_sem).wait()


def share(mine, span_x, span_y):
    inside = pl.BlockSpec(memory_space=pltpu.VMEM)
    return pl.pallas_call(
        functools.partial(share_kernel, span_x, span_y),
        in_specs=[inside],
        out_specs=inside,
        out_shape=jax.ShapeDtypeStruct((span_x * span_y,) + mine.shape, mine.dtype),
        scratch_shapes=[pltpu.SemaphoreType.DMA] * 3,
        compiler_params=pltpu.CompilerParams(collective_id=1, has_side_effects=True),
        name="share",
    )(mine)


def exchange_kernel(
    span_x, span_y, growth, capacity, log_crit, bins_ref, live_ref, route_ref, table_ref, rise_ref,
    source_ref, place_ref, cy_high, cy_low, cx_high, cx_low,
    recomb, out, load_ref,
    field, buf, known, coefs, sums, loads, load_parts, own, line, packed, arrived, stage,
    high, low, field_sems, recomb_sem,
    first_send, first_recv, first_own, line_send, line_recv, far_send, far_recv,
    back_send, back_recv, back_own, load_sems,
):
    steps, group, cells_y, cells_x = buf.shape
    depth_all = steps * group
    size_y, size_x = high.shape
    tiles = source_ref.shape[1]
    edge = depth_all // tiles
    per_tile = steps // tiles
    pairs = len(growth)
    part = group // span_x
    rows = part * cells_y
    per = 128 // edge
    packs = packed.shape[1]
    lane_blocks = size_x // 128
    block = 128
    gx, gy = lax.axis_index("gx"), lax.axis_index("gy")
    level, w = gy // part, lax.rem(gy, part)
    half, side = level // 2, lax.rem(level, 2)
    mate = 2 * half + 1 - side
    me = gx * part + w
    is_middle = (level == 1) | (level == 2)
    is_end = (level == 0) | (level == 3)

    def at(i, j):
        return {"gx": i, "gy": j}

    def place(ref, s, i, j):
        return ref.at[
            s,
            pl.ds(pl.multiple_of(j * cells_y, cells_y), cells_y),
            pl.ds(pl.multiple_of(i * cells_x, cells_x), cells_x),
        ]

    def each_of_level(act):
        def body(n, carry):
            act(lax.rem(gx + n // part, span_x), lax.rem(w + n % part, part))
            return carry

        lax.fori_loop(1, group, body, 0)

    def every_peer(act):
        def body(n, carry):
            act(lax.rem(gx + n // span_y, span_x), lax.rem(gy + n % span_y, span_y))
            return carry

        lax.fori_loop(1, span_x * span_y, body, 0)

    barrier = pltpu.get_barrier_semaphore()
    every_peer(
        lambda i, j: pl.semaphore_signal(barrier, inc=1, device_id=at(i, j), device_id_type=MESH)
    )
    fetches = field_sems.shape[0]
    fetch_rows = cells_y // fetches

    def fetch(n):
        part_rows = pl.ds(n * fetch_rows, fetch_rows)
        return pltpu.make_async_copy(
            log_crit.at[:, part_rows], field.at[:, part_rows], field_sems.at[n]
        )

    for n in range(fetches):
        fetch(n).start()

    def first(s):
        def act(i, j):
            pltpu.make_async_remote_copy(
                src_ref=buf.at[s, i * part + j],
                dst_ref=place(own, s, gx, w),
                send_sem=first_send.at[s],
                recv_sem=first_recv.at[s],
                device_id=at(i, level * part + j),
                device_id_type=MESH,
            ).start()

        each_of_level(act)
        pltpu.make_async_copy(buf.at[s, me], place(own, s, gx, w), first_own.at[s]).start()

    def send_back(s):
        def act(i, j):
            pltpu.make_async_remote_copy(
                src_ref=place(line, s, i, j),
                dst_ref=out.at[s, me],
                send_sem=back_send.at[s],
                recv_sem=back_recv.at[s],
                device_id=at(i, level * part + j),
                device_id_type=MESH,
            ).start()

        each_of_level(act)
        pltpu.make_async_copy(place(line, s, gx, w), out.at[s, me], back_own.at[s]).start()

    def to_mate(source, s):
        return pltpu.make_async_remote_copy(
            src_ref=source.at[s],
            dst_ref=line.at[s],
            send_sem=line_send.at[s],
            recv_sem=line_recv.at[s],
            device_id=at(gx, mate * part + w),
            device_id_type=MESH,
        )

    def to_far(s):
        return pltpu.make_async_remote_copy(
            src_ref=packed.at[s],
            dst_ref=arrived.at[s],
            send_sem=far_send.at[s],
            recv_sem=far_recv.at[s],
            device_id=at(gx, (3 - level) * part + w),
            device_id_type=MESH,
        )

    def wait_others(sem, s):
        some = buf.at[0, pl.ds(0, group - 1)]
        pltpu.make_async_copy(some, some, sem.at[s]).wait()

    def wait_own(sem, s):
        one = buf.at[0, 0]
        pltpu.make_async_copy(one, one, sem.at[s]).wait()

    def wait_plane(sem, s):
        pltpu.make_async_copy(own.at[s], own.at[s], sem.at[s]).wait()

    def wait_packed(sem, s):
        pltpu.make_async_copy(packed.at[s], packed.at[s], sem.at[s]).wait()

    def unrolled(count, width, act):
        def some(n, carry):
            for r in range(width):
                act(n * width + r)
            return carry

        lax.fori_loop(0, count // width, some, 0)
        for n in range(count // width * width, count):
            act(n)

    def eight(n):
        return pl.ds(pl.multiple_of(n * 8, 8), 8)

    def turn_in():
        def one(n, carry):
            value = turned(field[:, eight(n), :])
            buf[:, :, eight(n), :] = value.reshape(steps, group, 8, cells_x)
            return carry

        lax.fori_loop(0, cells_y // 8, one, 0)

    def turn_out(n):
        value = buf[:, :, eight(n), :].reshape(depth_all, 8, cells_x)
        field[:, eight(n), :] = turned(value)

    def tabulate():
        rates = table_ref[...].astype(jnp.float32)
        upper, lower = rates[:pairs], rates[pairs:]
        known[:pairs] = upper + lower
        known[pairs:] = upper * rise_ref[1] + lower * rise_ref[0]

    def gather(t):
        def one(n, carry):
            kinds = bins_ref[t, eight(n), :]
            live = jnp.broadcast_to(live_ref[t, pl.ds(n * 8 // edge, 1), :], kinds.shape)
            for p in range(2 * pairs):
                row = jnp.broadcast_to(known[pl.ds(p, 1), :], kinds.shape)
                coefs[p, eight(n), :] = live * jnp.take_along_axis(
                    row, kinds, axis=1, mode="promise_in_bounds"
                )
            return carry

        lax.fori_loop(0, cells_y // 8, one, 0)
        sums[t] = jnp.zeros(sums.shape[1:], jnp.float32)

    def evaluate(s):
        t = s // per_tile
        batch = 4

        def one(n, carry):
            rows = pl.ds(pl.multiple_of(n // (group // batch) * 8, 8), 8)
            planes = pl.ds(n % (group // batch) * batch, batch)
            value = integral(
                buf[s, planes, rows, :], growth,
                lambda p: coefs[p, rows, :], lambda p: coefs[pairs + p, rows, :],
            )
            buf[s, planes, rows, :] = value
            sums[t, rows, :] += jnp.sum(value, axis=0)
            return carry

        lax.fori_loop(0, cells_y // 8 * (group // batch), one, 0)

    def send_loads():
        blocks_y = live_ref.shape[1]
        lines = [
            jnp.sum(sums[t, b * edge : (b + 1) * edge, :], axis=0, keepdims=True)
            for t in range(tiles)
            for b in range(blocks_y)
        ]
        for g in range(span_y):
            share_of = None
            for n, line_sum in enumerate(lines):
                chosen = jnp.where(route_ref[pl.ds(n, 1), :] == g, line_sum, 0.0)
                share_of = chosen if share_of is None else share_of + chosen
            total = jnp.sum(share_of, axis=1, keepdims=True) / (edge * edge * edge) / capacity
            loads[g] = jnp.broadcast_to(total, (8, 128))
        pltpu.make_async_copy(loads.at[gy], load_parts.at[gy], load_sems.at[2]).start()

        def send(n, carry):
            j = lax.rem(gy + n, span_y)
            pltpu.make_async_remote_copy(
                src_ref=loads.at[j],
                dst_ref=load_parts.at[gy],
                send_sem=load_sems.at[0],
                recv_sem=load_sems.at[1],
                device_id=at(gx, j),
                device_id_type=MESH,
            ).start()
            return carry

        lax.fori_loop(1, span_y, send, 0)

    lane = lax.broadcasted_iota(jnp.int32, (edge, 128), 1)

    def rows_at(start, count):
        return pl.ds(pl.multiple_of(start, count), count)

    def turns(value):
        return [value if r == 0 else pltpu.roll(value, r * edge, 1) for r in range(per)]

    def pack(s):
        strip = rows // edge * lane_blocks

        def fill(n):
            across = pl.ds(pl.multiple_of(n % lane_blocks * 128, 128), 128)
            chunk = rows_at(n // lane_blocks * edge, edge)
            for r, value in enumerate(turns(own[s, chunk, across])):
                stage[(side * strip + n) * per + r] = value
            for r, value in enumerate(turns(line[s, chunk, across])):
                stage[((1 - side) * strip + n) * per + r] = value

        unrolled(strip, 2, fill)
        t = s // per_tile

        def one(g):
            total = None
            for q in range(per):
                piece = stage[source_ref[half, t, g * per + q]]
                total = piece if total is None else jnp.where(lane >= q * edge, piece, total)
            packed[s, g] = total

        unrolled(packs, 4, one)

    def unpack(s):
        for r in range(per):
            stage[r] = jnp.zeros((edge, 128), jnp.float32)

        def fill(g):
            for r, value in enumerate(turns(arrived[s, g])):
                stage[(g + 1) * per + r] = value

        unrolled(packs, 4, fill)
        t = s // per_tile

        def one(n):
            down, block_x = n // lane_blocks, lax.rem(n, lane_blocks)
            total = None
            for q in range(per):
                piece = stage[place_ref[1 - half, t, n * per + q]]
                total = piece if total is None else jnp.where(lane >= q * edge, piece, total)
            to = (
                rows_at((1 - half) * 2 * rows + down * edge, edge),
                rows_at(block_x * 128, 128),
            )
            high[to], low[to] = halves(total)

        unrolled(2 * rows // edge * lane_blocks, 4, one)

    def split(source, s, which):
        def one(r, carry):
            to = rows_at(which * rows + r * block, block)
            high[to, :], low[to, :] = halves(source[s, rows_at(r * block, block), :])
            return carry

        lax.fori_loop(0, rows // block, one, 0)

    def along_y(which, r):
        chunk = rows_at(which * rows + r * block, block)
        return dot3(cy_high[chunk, :], cy_low[chunk, :], high[...], low[...])

    def along_x(value):
        return dot3(*halves(value), cx_high[...], cx_low[...])

    def middle_first(s):
        wait_own(first_own, s)
        wait_others(first_recv, s)
        wait_plane(line_recv, s)
        pack(s)
        to_far(s).start()

    def middle_second(s):
        split(own, s, level)
        split(line, s, mate)
        wait_packed(far_recv, s)
        unpack(s)

        def for_mate(r, carry):
            own[s, rows_at(r * block, block), :] = along_y(mate, r)
            return carry

        lax.fori_loop(0, rows // block, for_mate, 0)
        to_mate(own, s).start()

        def for_me(r, carry):
            line[s, rows_at(r * block, block), :] = along_x(along_y(level, r))
            return carry

        lax.fori_loop(0, rows // block, for_me, 0)
        send_back(s)

    def end_first(s):
        wait_own(first_own, s)
        wait_others(first_recv, s)
        to_mate(own, s).start()

    def end_second(s):
        wait_plane(line_recv, s)

        def for_me(r, carry):
            line[s, rows_at(r * block, block), :] = along_x(line[s, rows_at(r * block, block), :])
            return carry

        lax.fori_loop(0, rows // block, for_me, 0)
        send_back(s)

    lags = (2, 3, 5, 7)
    out_rounds = 4

    def at_step(i, who, lag, act):
        @pl.when(who & (i >= lag) & (i < steps + lag))
        def _():
            act(i - lag)

    def body(i, carry):
        at_step(i, is_end, lags[0], end_first)

        @pl.when((i < steps) & (i % per_tile == 0))
        def _():
            gather(i // per_tile)

        @pl.when(i < steps)
        def _():
            evaluate(i)

        @pl.when(i < steps)
        def _():
            first(i)

        at_step(i, is_middle, lags[1], middle_first)
        at_step(i, is_middle, lags[2], middle_second)
        at_step(i, is_end, lags[3], end_second)

        @pl.when(i == steps)
        def _():
            send_loads()

        @pl.when((i >= steps) & (i < steps + out_rounds))
        def _():
            for n in range(cells_y // 8 // out_rounds):
                turn_out((i - steps) * (cells_y // 8 // out_rounds) + n)

        return carry

    last = max(lags[3], out_rounds)
    tabulate()
    for n in range(fetches):
        fetch(n).wait()
    turn_in()
    pl.semaphore_wait(barrier, span_x * span_y - 1)
    lax.fori_loop(0, steps + last, body, 0)
    write = pltpu.make_async_copy(field, recomb, recomb_sem)
    write.start()

    @pl.when(is_middle)
    def _():
        def drain(s, carry):
            wait_packed(far_send, s)
            return carry

        lax.fori_loop(0, steps, drain, 0)

    some_loads = loads.at[pl.ds(0, span_y - 1)]
    pltpu.make_async_copy(some_loads, some_loads, load_sems.at[0]).wait()
    pltpu.make_async_copy(some_loads, some_loads, load_sems.at[1]).wait()
    pltpu.make_async_copy(loads.at[0], loads.at[0], load_sems.at[2]).wait()
    load_ref[...] = jnp.sum(load_parts[...], axis=0)

    def finish(s, carry):
        wait_plane(line_send, s)
        wait_others(first_send, s)
        wait_others(back_send, s)
        wait_own(back_own, s)
        wait_others(back_recv, s)
        return carry

    lax.fori_loop(0, steps, finish, 0)
    write.wait()


def exchange(
    slots, collective, span_x, span_y, growth, capacity, log_crit, bins, live, routes, table, rise,
    source, position, cy_high, cy_low, cx_high, cx_low,
):
    cells_x, cells_y, depth_all = log_crit.shape
    group = span_x * span_y // levels
    steps = depth_all // group
    edge = depth_all // source.shape[1]
    size_y, size_x = cy_high.shape[0], cx_high.shape[0]
    rows = size_y // levels
    packs = slots * edge // 128
    per = 128 // edge
    stage_size = max(2 * rows * size_x // edge // edge, per * (packs + 1))
    anywhere = pl.BlockSpec(memory_space=pl.ANY)
    inside = pl.BlockSpec(memory_space=pltpu.VMEM)
    scalars = pl.BlockSpec(memory_space=pltpu.SMEM)
    planes = pltpu.VMEM((steps, rows, size_x), jnp.float32)
    packing = pltpu.VMEM((steps, packs, edge, 128), jnp.float32)
    parts = pltpu.VMEM((span_y, 8, 128), jnp.float32)
    halved = pltpu.VMEM((size_y, size_x), jnp.bfloat16)
    sems = pltpu.SemaphoreType.DMA((steps,))
    plane_bytes = 4 * steps * rows * size_x
    held = (
        4 * plane_bytes + 8 * steps * slots * edge * edge + 4 * stage_size * edge * 128
        + 12 * size_y * size_x + 8 * len(growth) * cells_y * cells_x
    )
    return pl.pallas_call(
        functools.partial(exchange_kernel, span_x, span_y, growth, capacity),
        in_specs=[anywhere] + [inside] * 5 + [scalars] * 2 + [inside] * 4,
        out_specs=[anywhere] * 2 + [inside],
        out_shape=[
            jax.ShapeDtypeStruct(log_crit.shape, jnp.float32),
            jax.ShapeDtypeStruct((steps, group, cells_y, cells_x), jnp.float32),
            jax.ShapeDtypeStruct((8, 128), jnp.float32),
        ],
        scratch_shapes=[
            pltpu.VMEM(log_crit.shape, jnp.float32),
            pltpu.VMEM((steps, group, cells_y, cells_x), jnp.float32),
            pltpu.VMEM(table.shape, jnp.float32),
            pltpu.VMEM((2 * len(growth), cells_y, cells_x), jnp.float32),
            pltpu.VMEM((source.shape[1], cells_y, cells_x), jnp.float32),
            parts,
            parts,
            planes,
            planes,
            packing,
            packing,
            pltpu.VMEM((stage_size, edge, 128), jnp.float32),
            halved,
            halved,
            pltpu.SemaphoreType.DMA((4,)),
            pltpu.SemaphoreType.DMA,
        ]
        + [sems] * 10
        + [pltpu.SemaphoreType.DMA((3,))],
        compiler_params=pltpu.CompilerParams(
            collective_id=collective, has_side_effects=True,
            vmem_limit_bytes=min(held + held // 16 + 2 * 1024 * 1024, vmem_grant),
        ),
        name=f"exchange{slots}",
    )(
        log_crit, bins, live, routes, table, rise, source, position, cy_high, cy_low, cx_high,
        cx_low,
    )


def slot_tables(masks, edge):
    halves_count = 2
    flat = masks.reshape(halves_count, -1, masks.shape[2]).transpose(0, 2, 1)
    slots = flat.shape[2]
    before = jnp.triu(jnp.ones((slots, slots), jnp.bfloat16), 1)
    rank = jnp.dot(flat.astype(jnp.bfloat16), before, preferred_element_type=jnp.float32)
    rank = rank.astype(jnp.int32)
    per = 128 // edge
    indices = jnp.arange(slots, dtype=jnp.int32)
    shifted = (indices % per - rank) % per
    position = jnp.where(flat == 1, rank, -1)
    place = jnp.where(flat == 1, (rank // per + 1) * per + shifted, 0)
    from_place = indices // per * per + (rank - indices) % per
    source = jnp.sum(
        jnp.where(position[:, :, None, :] == indices[:, None], from_place[:, :, None, :], 0), axis=3
    )
    most = jnp.max(jnp.sum(flat, axis=2))
    return source, place, most


def turned(value):
    flat = jnp.swapaxes(value, 0, 1)
    return jnp.swapaxes(jnp.stack([flat[r].T for r in range(8)]), 0, 1)


def turn_kernel(source_ref, kept_ref, out_ref, kept_out):
    for row in range(0, source_ref.shape[1], 8):
        out_ref[:, row : row + 8, :] = turned(source_ref[:, row : row + 8, :])
    kept_out[...] = kept_ref[...]


def turn(source, kept):
    depth_all, cells_y, cells_x = source.shape
    rows = 8
    planes = pl.BlockSpec((depth_all, rows, cells_x), lambda j: (0, j, 0))
    cells = pl.BlockSpec((cells_x, rows, depth_all), lambda j: (0, j, 0))
    shape = jax.ShapeDtypeStruct((cells_x, cells_y, depth_all), jnp.float32)
    return pl.pallas_call(
        turn_kernel,
        grid=(cells_y // rows,),
        in_specs=[planes, cells],
        out_specs=[cells, cells],
        out_shape=[shape, shape],
        compiler_params=pltpu.CompilerParams(vmem_limit_bytes=16 * 1024 * 1024),
        name="turn",
    )(source, kept)


def wave_freq(length):
    half = length // 2
    return np.concatenate([np.arange(half + 1), np.arange(1, half)])


def wave_table(length):
    indices = np.arange(length)
    turns = indices[:, None] * wave_freq(length)[None, :] % length
    shift = np.where(indices < length // 2 + 1, 0.0, math.pi / 2)[None, :]
    return jnp.asarray(np.cos(2.0 * math.pi / length * turns - shift), jnp.float32)


def circulant(gain, table):
    length = gain.shape[0]
    half = length // 2
    freq = wave_freq(length)
    weight = jnp.concatenate([gain[: half + 1], gain[1:half]])
    doubled = jnp.asarray(np.where((freq == 0) | (freq == half), 1.0, 2.0), jnp.float32)
    scaled = lax.optimization_barrier(table * (weight * doubled / length))
    return lax.dot_general(
        scaled, table, (((1,), (1,)), ((), ())), precision=lax.Precision.HIGHEST
    )


def on_device(log_crit, col_bins, rate_table, tile_mask, tile_route, filt_x, filt_y):
    blocks_x, blocks_y, tiles = tile_mask.shape
    cells_x, cells_y, depth_all = log_crit.shape
    edge = cells_x // blocks_x
    span_x, span_y = lax.axis_size("gx"), lax.axis_size("gy")
    devices = span_x * span_y
    nodes = rate_table.shape[1]
    half = nodes // 2

    bins = col_bins.transpose(2, 1, 0)
    live = jnp.repeat((tile_mask == 1).astype(jnp.float32).transpose(2, 1, 0), edge, axis=2)
    routes = jnp.repeat(
        tile_route.transpose(2, 1, 0).reshape(tiles * blocks_y, blocks_x), edge, axis=1
    )
    table = jnp.concatenate([rate_table[:, half:], rate_table[:, half - 1 :: -1]], axis=1).T

    growth = node_growth(nodes)
    ends = np.array([growth, [1.0 / e for e in growth]], np.float32)
    rise = jnp.asarray(np.broadcast_to(ends[:, :, None], (2, half, table.shape[1])))
    capacity = blocks_x * blocks_y * tiles // 2
    table_x = wave_table(filt_x.shape[0])
    table_y = table_x if filt_y.shape == filt_x.shape else wave_table(filt_y.shape[0])
    mine = jnp.pad((tile_mask == 1).astype(jnp.int32).reshape(1, -1), ((0, 7), (0, 128 - blocks_x * blocks_y * tiles)))
    masks = share(mine, span_x, span_y)[:, 0, : blocks_x * blocks_y * tiles]
    masks = masks.reshape(span_x, span_y, blocks_x, blocks_y, tiles).transpose(1, 3, 0, 2, 4)
    masks = masks.reshape(span_y * blocks_y, span_x * blocks_x, tiles)
    source, position, most = slot_tables(masks, edge)
    every = position.shape[2]
    few = every * 19 // 32
    operands = (
        log_crit, bins, live, routes, table, rise, source, position,
        *outer_halves(circulant(filt_y, table_y)), *outer_halves(circulant(filt_x, table_x)),
    )

    def run(slots, collective):
        return lambda *args: exchange(slots, collective, span_x, span_y, growth, capacity, *args)

    recomb, back, device_load = lax.cond(most <= few, run(few, 2), run(every, 3), *operands)
    smoothed, recomb = turn(back.reshape(depth_all, cells_y, cells_x), recomb)
    return (recomb, smoothed, device_load[:1, :1])


def solution(mesh):
    placed = (
        P("gx", "gy", None),
        P("gx", "gy", None),
        P(),
        P("gx", "gy", None),
        P("gx", "gy", None),
        P(),
        P(),
    )
    return jax.shard_map(
        on_device,
        mesh=mesh,
        in_specs=placed,
        out_specs=(P("gx", "gy", None), P("gx", "gy", None), P("gx", "gy")),
        check_vma=False,
    )
```

```python
import functools
import math

import jax
import jax.numpy as jnp
import numpy as np
from jax import lax
from jax.experimental import pallas as pl
from jax.experimental.pallas import tpu as pltpu
from jax.sharding import PartitionSpec as P

steepness = 3.0
vmem_grant = 60 * 1024 * 1024
MESH = pl.DeviceIdType.MESH
levels = 4


def node_growth(nodes):
    return [math.exp(steepness * (-2.5 + 5.0 * q / (nodes - 1))) for q in range(nodes // 2, nodes)]


def join(left, right):
    num_left, den_left = left
    num_right, den_right = right
    return (num_left * den_right + num_right * den_left, den_left * den_right)


def integral(field, growth, coef_a, coef_b):
    pairs = len(growth)
    v = jnp.exp(field * steepness)
    y = v + jnp.exp(field * -steepness)
    total = None
    for first in range(0, pairs, 4):
        terms = []
        for p in range(first, min(first + 4, pairs)):
            num = coef_a(p) * v + coef_b(p)
            terms.append((num, y + (growth[p] + 1.0 / growth[p])))
        while len(terms) > 1:
            terms = [
                join(terms[i], terms[i + 1]) if i + 1 < len(terms) else terms[i]
                for i in range(0, len(terms), 2)
            ]
        part = terms[0][0] * (1.0 / terms[0][1])
        total = part if total is None else total + part
    return total


def halves(value):
    high = value.astype(jnp.bfloat16)
    return high, (value - high.astype(jnp.float32)).astype(jnp.bfloat16)


def outer_halves(value):
    high = lax.reduce_precision(value, 8, 7)
    low = lax.reduce_precision(value - high, 8, 7)
    return high.astype(jnp.bfloat16), low.astype(jnp.bfloat16)


def dot3(a_high, a_low, b_high, b_low):
    dot = functools.partial(jnp.dot, preferred_element_type=jnp.float32)
    return dot(a_high, b_high) + (dot(a_high, b_low) + dot(a_low, b_high))


def exchange_kernel(
    span_x, span_y, growth, capacity, log_crit, bins_ref, live_ref, route_ref, table_ref, rise_ref,
    mask_ref, cy_high, cy_low, cx_high, cx_low,
    recomb, out, load_ref, most_ref,
    field, buf, known, coefs, sums, loads, load_parts, own, line, packed, arrived, stage,
    high, low, masks, made, source_ref, place_ref, field_sems, recomb_sem, mask_sems,
    first_send, first_recv, first_own, line_send, line_recv, far_send, far_recv,
    back_send, back_recv, back_own, load_sems,
):
    steps, group, cells_y, cells_x = buf.shape
    depth_all = steps * group
    size_y, size_x = high.shape
    tiles = bins_ref.shape[0]
    edge = depth_all // tiles
    per_tile = steps // tiles
    pairs = len(growth)
    part = group // span_x
    rows = part * cells_y
    per = 128 // edge
    packs = packed.shape[1]
    lane_blocks = size_x // 128
    block = 128
    gx, gy = lax.axis_index("gx"), lax.axis_index("gy")
    level, w = gy // part, lax.rem(gy, part)
    half, side = level // 2, lax.rem(level, 2)
    mate = 2 * half + 1 - side
    me = gx * part + w
    is_middle = (level == 1) | (level == 2)
    is_end = (level == 0) | (level == 3)

    def at(i, j):
        return {"gx": i, "gy": j}

    def place(ref, s, i, j):
        return ref.at[
            s,
            pl.ds(pl.multiple_of(j * cells_y, cells_y), cells_y),
            pl.ds(pl.multiple_of(i * cells_x, cells_x), cells_x),
        ]

    def each_of_level(act):
        def body(n, carry):
            act(lax.rem(gx + n // part, span_x), lax.rem(w + n % part, part))
            return carry

        lax.fori_loop(1, group, body, 0)

    def every_peer(act):
        def body(n, carry):
            act(lax.rem(gx + n // span_y, span_x), lax.rem(gy + n % span_y, span_y))
            return carry

        lax.fori_loop(1, span_x * span_y, body, 0)

    barrier = pltpu.get_barrier_semaphore()
    every_peer(
        lambda i, j: pl.semaphore_signal(barrier, inc=1, device_id=at(i, j), device_id_type=MESH)
    )
    fetches = field_sems.shape[0]
    fetch_rows = cells_y // fetches

    def fetch(n):
        part_rows = pl.ds(n * fetch_rows, fetch_rows)
        return pltpu.make_async_copy(
            log_crit.at[:, part_rows], field.at[:, part_rows], field_sems.at[n]
        )

    for n in range(fetches):
        fetch(n).start()

    me_all = gx * span_y + gy

    def send_mask(i, j):
        pltpu.make_async_remote_copy(
            src_ref=mask_ref,
            dst_ref=masks.at[me_all],
            send_sem=mask_sems.at[0],
            recv_sem=mask_sems.at[1],
            device_id=at(i, j),
            device_id_type=MESH,
        ).start()

    def tables():
        some = masks.at[pl.ds(0, span_x * span_y - 1)]
        pltpu.make_async_copy(some, some, mask_sems.at[0]).wait()
        pltpu.make_async_copy(some, some, mask_sems.at[1]).wait()
        pltpu.make_async_copy(mask_ref, mask_ref, mask_sems.at[2]).wait()
        blocks_y, blocks_x = live_ref.shape[1], cells_x // edge
        slots = source_ref.shape[1]
        across = size_x // edge

        def numbers(shape, axis):
            return lax.broadcasted_iota(jnp.int32, shape, axis)

        flags = masks[:, 0, :].astype(jnp.bfloat16)
        held = jnp.zeros((slots, 128), jnp.float32)
        slot = numbers((slots, 128), 0)
        column = numbers((slots, 128), 1)
        down, over = slot // across, slot % across
        lane_of = (over % blocks_x * blocks_y + down % blocks_y) * tiles
        owner = numbers((slots, span_x * span_y), 0)
        owner = owner % across // blocks_x * span_y + owner // across // blocks_y
        device = numbers((slots, span_x * span_y), 1)
        for h in range(2):
            chosen = jnp.where(owner + h * (span_y // 2) == device, 1.0, 0.0).astype(jnp.bfloat16)
            picked = jnp.dot(chosen, flags, preferred_element_type=jnp.float32)
            for t in range(tiles):
                value = jnp.sum(
                    jnp.where(column == lane_of + t, picked, 0.0), axis=1, keepdims=True
                )
                held = jnp.where(column == h * tiles + t, value, held)
        later = numbers((slots, slots), 0) > numbers((slots, slots), 1)
        before = jnp.where(later, 1.0, 0.0).astype(jnp.bfloat16)
        rank = jnp.dot(before, held.astype(jnp.bfloat16), preferred_element_type=jnp.float32)
        rank = rank.astype(jnp.int32)
        live = held > 0.5
        shift = (slot % per + per - rank % per) % per
        places = jnp.where(live, (rank // per + 1) * per + shift, 0)
        made[1] = places.T[: 2 * tiles]
        rank = jnp.where(live, rank, -1)
        to = numbers((slots, slots), 1)
        origin = numbers((slots, slots), 0)
        origin = origin // per * per + (to % per + per - origin % per) % per
        for e in range(2 * tiles):
            made[0, e : e + 1] = jnp.sum(
                jnp.where(rank[:, e : e + 1] == to, origin, 0), axis=0, keepdims=True
            )
        most = jnp.max(jnp.sum(held, axis=0, keepdims=True), axis=1, keepdims=True)
        most_ref[...] = jnp.broadcast_to(most, (8, 128))
        for n, table in enumerate((source_ref, place_ref)):
            copy = pltpu.make_async_copy(made.at[n], table, mask_sems.at[3 + n])
            copy.start()
            copy.wait()

    def first(s):
        def act(i, j):
            pltpu.make_async_remote_copy(
                src_ref=buf.at[s, i * part + j],
                dst_ref=place(own, s, gx, w),
                send_sem=first_send.at[s],
                recv_sem=first_recv.at[s],
                device_id=at(i, level * part + j),
                device_id_type=MESH,
            ).start()

        each_of_level(act)
        pltpu.make_async_copy(buf.at[s, me], place(own, s, gx, w), first_own.at[s]).start()

    def send_back(s):
        def act(i, j):
            pltpu.make_async_remote_copy(
                src_ref=place(line, s, i, j),
                dst_ref=out.at[s, me],
                send_sem=back_send.at[s],
                recv_sem=back_recv.at[s],
                device_id=at(i, level * part + j),
                device_id_type=MESH,
            ).start()

        each_of_level(act)
        pltpu.make_async_copy(place(line, s, gx, w), out.at[s, me], back_own.at[s]).start()

    def to_mate(source, s):
        return pltpu.make_async_remote_copy(
            src_ref=source.at[s],
            dst_ref=line.at[s],
            send_sem=line_send.at[s],
            recv_sem=line_recv.at[s],
            device_id=at(gx, mate * part + w),
            device_id_type=MESH,
        )

    def to_far(s):
        return pltpu.make_async_remote_copy(
            src_ref=packed.at[s],
            dst_ref=arrived.at[s],
            send_sem=far_send.at[s],
            recv_sem=far_recv.at[s],
            device_id=at(gx, (3 - level) * part + w),
            device_id_type=MESH,
        )

    def wait_others(sem, s):
        some = buf.at[0, pl.ds(0, group - 1)]
        pltpu.make_async_copy(some, some, sem.at[s]).wait()

    def wait_own(sem, s):
        one = buf.at[0, 0]
        pltpu.make_async_copy(one, one, sem.at[s]).wait()

    def wait_plane(sem, s):
        pltpu.make_async_copy(own.at[s], own.at[s], sem.at[s]).wait()

    def wait_packed(sem, s):
        pltpu.make_async_copy(packed.at[s], packed.at[s], sem.at[s]).wait()

    def unrolled(count, width, act):
        def some(n, carry):
            for r in range(width):
                act(n * width + r)
            return carry

        lax.fori_loop(0, count // width, some, 0)
        for n in range(count // width * width, count):
            act(n)

    def eight(n):
        return pl.ds(pl.multiple_of(n * 8, 8), 8)

    def turn_in():
        def one(n, carry):
            value = turned(field[:, eight(n), :])
            buf[:, :, eight(n), :] = value.reshape(steps, group, 8, cells_x)
            return carry

        lax.fori_loop(0, cells_y // 8, one, 0)

    def turn_out(n):
        value = buf[:, :, eight(n), :].reshape(depth_all, 8, cells_x)
        field[:, eight(n), :] = turned(value)

    def tabulate():
        rates = table_ref[...].astype(jnp.float32)
        upper, lower = rates[:pairs], rates[pairs:]
        known[:pairs] = upper + lower
        known[pairs:] = upper * rise_ref[1] + lower * rise_ref[0]

    def gather(t):
        def one(n, carry):
            kinds = bins_ref[t, eight(n), :]
            live = jnp.broadcast_to(live_ref[t, pl.ds(n * 8 // edge, 1), :], kinds.shape)
            for p in range(2 * pairs):
                row = jnp.broadcast_to(known[pl.ds(p, 1), :], kinds.shape)
                coefs[p, eight(n), :] = live * jnp.take_along_axis(
                    row, kinds, axis=1, mode="promise_in_bounds"
                )
            return carry

        lax.fori_loop(0, cells_y // 8, one, 0)
        sums[t] = jnp.zeros(sums.shape[1:], jnp.float32)

    def evaluate(s):
        t = s // per_tile
        batch = 4

        def one(n, carry):
            rows = pl.ds(pl.multiple_of(n // (group // batch) * 8, 8), 8)
            planes = pl.ds(n % (group // batch) * batch, batch)
            value = integral(
                buf[s, planes, rows, :], growth,
                lambda p: coefs[p, rows, :], lambda p: coefs[pairs + p, rows, :],
            )
            buf[s, planes, rows, :] = value
            sums[t, rows, :] += jnp.sum(value, axis=0)
            return carry

        lax.fori_loop(0, cells_y // 8 * (group // batch), one, 0)

    def send_loads():
        blocks_y = live_ref.shape[1]
        lines = [
            jnp.sum(sums[t, b * edge : (b + 1) * edge, :], axis=0, keepdims=True)
            for t in range(tiles)
            for b in range(blocks_y)
        ]
        for g in range(span_y):
            share_of = None
            for n, line_sum in enumerate(lines):
                chosen = jnp.where(route_ref[pl.ds(n, 1), :] == g, line_sum, 0.0)
                share_of = chosen if share_of is None else share_of + chosen
            total = jnp.sum(share_of, axis=1, keepdims=True) / (edge * edge * edge) / capacity
            loads[g] = jnp.broadcast_to(total, (8, 128))
        pltpu.make_async_copy(loads.at[gy], load_parts.at[gy], load_sems.at[2]).start()

        def send(n, carry):
            j = lax.rem(gy + n, span_y)
            pltpu.make_async_remote_copy(
                src_ref=loads.at[j],
                dst_ref=load_parts.at[gy],
                send_sem=load_sems.at[0],
                recv_sem=load_sems.at[1],
                device_id=at(gx, j),
                device_id_type=MESH,
            ).start()
            return carry

        lax.fori_loop(1, span_y, send, 0)

    lane = lax.broadcasted_iota(jnp.int32, (edge, 128), 1)

    def rows_at(start, count):
        return pl.ds(pl.multiple_of(start, count), count)

    def turns(value):
        return [value if r == 0 else pltpu.roll(value, r * edge, 1) for r in range(per)]

    def inside(index):
        return jnp.clip(index, 0, stage.shape[0] - 1)

    def pack(s):
        strip = rows // edge * lane_blocks

        def fill(n):
            across = pl.ds(pl.multiple_of(n % lane_blocks * 128, 128), 128)
            chunk = rows_at(n // lane_blocks * edge, edge)
            for r, value in enumerate(turns(own[s, chunk, across])):
                stage[(side * strip + n) * per + r] = value
            for r, value in enumerate(turns(line[s, chunk, across])):
                stage[((1 - side) * strip + n) * per + r] = value

        unrolled(strip, 2, fill)
        t = s // per_tile

        def one(g):
            total = None
            for q in range(per):
                piece = stage[inside(source_ref[half * tiles + t, g * per + q])]
                total = piece if total is None else jnp.where(lane >= q * edge, piece, total)
            packed[s, g] = total

        unrolled(packs, 4, one)

    def unpack(s):
        for r in range(per):
            stage[r] = jnp.zeros((edge, 128), jnp.float32)

        def fill(g):
            for r, value in enumerate(turns(arrived[s, g])):
                stage[(g + 1) * per + r] = value

        unrolled(packs, 4, fill)
        t = s // per_tile

        def one(n):
            down, block_x = n // lane_blocks, lax.rem(n, lane_blocks)
            total = None
            for q in range(per):
                piece = stage[inside(place_ref[(1 - half) * tiles + t, n * per + q])]
                total = piece if total is None else jnp.where(lane >= q * edge, piece, total)
            to = (
                rows_at((1 - half) * 2 * rows + down * edge, edge),
                rows_at(block_x * 128, 128),
            )
            high[to], low[to] = halves(total)

        unrolled(2 * rows // edge * lane_blocks, 4, one)

    def split(source, s, which):
        def one(r, carry):
            to = rows_at(which * rows + r * block, block)
            high[to, :], low[to, :] = halves(source[s, rows_at(r * block, block), :])
            return carry

        lax.fori_loop(0, rows // block, one, 0)

    def along_y(which, r):
        chunk = rows_at(which * rows + r * block, block)
        return dot3(cy_high[chunk, :], cy_low[chunk, :], high[...], low[...])

    def along_x(value):
        return dot3(*halves(value), cx_high[...], cx_low[...])

    def middle_first(s):
        wait_own(first_own, s)
        wait_others(first_recv, s)
        wait_plane(line_recv, s)
        pack(s)
        to_far(s).start()

    def middle_second(s):
        split(own, s, level)
        split(line, s, mate)
        wait_packed(far_recv, s)
        unpack(s)

        def for_mate(r, carry):
            own[s, rows_at(r * block, block), :] = along_y(mate, r)
            return carry

        lax.fori_loop(0, rows // block, for_mate, 0)
        to_mate(own, s).start()

        def for_me(r, carry):
            line[s, rows_at(r * block, block), :] = along_x(along_y(level, r))
            return carry

        lax.fori_loop(0, rows // block, for_me, 0)
        send_back(s)

    def end_first(s):
        wait_own(first_own, s)
        wait_others(first_recv, s)
        to_mate(own, s).start()

    def end_second(s):
        wait_plane(line_recv, s)

        def for_me(r, carry):
            line[s, rows_at(r * block, block), :] = along_x(line[s, rows_at(r * block, block), :])
            return carry

        lax.fori_loop(0, rows // block, for_me, 0)
        send_back(s)

    lags = (2, 3, 5, 7)
    out_rounds = 4

    def at_step(i, who, lag, act):
        @pl.when(who & (i >= lag) & (i < steps + lag))
        def _():
            act(i - lag)

    def body(i, carry):
        at_step(i, is_end, lags[0], end_first)

        @pl.when((i < steps) & (i % per_tile == 0))
        def _():
            gather(i // per_tile)

        @pl.when(i < steps)
        def _():
            evaluate(i)

        @pl.when(i < steps)
        def _():
            first(i)

        @pl.when(i == 1)
        def _():
            tables()

        at_step(i, is_middle, lags[1], middle_first)
        at_step(i, is_middle, lags[2], middle_second)
        at_step(i, is_end, lags[3], end_second)

        @pl.when(i == steps)
        def _():
            send_loads()

        @pl.when((i >= steps) & (i < steps + out_rounds))
        def _():
            for n in range(cells_y // 8 // out_rounds):
                turn_out((i - steps) * (cells_y // 8 // out_rounds) + n)

        return carry

    last = max(lags[3], out_rounds)
    tabulate()
    for n in range(fetches):
        fetch(n).wait()
    turn_in()
    pltpu.make_async_copy(mask_ref, masks.at[me_all], mask_sems.at[2]).start()
    pl.semaphore_wait(barrier, span_x * span_y - 1)
    every_peer(send_mask)
    lax.fori_loop(0, steps + last, body, 0)
    write = pltpu.make_async_copy(field, recomb, recomb_sem)
    write.start()

    @pl.when(is_middle)
    def _():
        def drain(s, carry):
            wait_packed(far_send, s)
            return carry

        lax.fori_loop(0, steps, drain, 0)

    some_loads = loads.at[pl.ds(0, span_y - 1)]
    pltpu.make_async_copy(some_loads, some_loads, load_sems.at[0]).wait()
    pltpu.make_async_copy(some_loads, some_loads, load_sems.at[1]).wait()
    pltpu.make_async_copy(loads.at[0], loads.at[0], load_sems.at[2]).wait()
    load_ref[...] = jnp.sum(load_parts[...], axis=0)

    def finish(s, carry):
        wait_plane(line_send, s)
        wait_others(first_send, s)
        wait_others(back_send, s)
        wait_own(back_own, s)
        wait_others(back_recv, s)
        return carry

    lax.fori_loop(0, steps, finish, 0)
    write.wait()


def exchange(
    slots, collective, span_x, span_y, growth, capacity, log_crit, bins, live, routes, table, rise,
    mask, cy_high, cy_low, cx_high, cx_low,
):
    cells_x, cells_y, depth_all = log_crit.shape
    group = span_x * span_y // levels
    steps = depth_all // group
    edge = depth_all // bins.shape[0]
    size_y, size_x = cy_high.shape[0], cx_high.shape[0]
    rows = size_y // levels
    packs = slots * edge // 128
    per = 128 // edge
    every = size_y // 2 // edge * (size_x // edge)
    stage_size = max(2 * rows * size_x // edge // edge, per * (packs + 1))
    anywhere = pl.BlockSpec(memory_space=pl.ANY)
    inside = pl.BlockSpec(memory_space=pltpu.VMEM)
    planes = pltpu.VMEM((steps, rows, size_x), jnp.float32)
    packing = pltpu.VMEM((steps, packs, edge, 128), jnp.float32)
    parts = pltpu.VMEM((span_y, 8, 128), jnp.float32)
    halved = pltpu.VMEM((size_y, size_x), jnp.bfloat16)
    sems = pltpu.SemaphoreType.DMA((steps,))
    plane_bytes = 4 * steps * rows * size_x
    held = (
        4 * plane_bytes + 8 * steps * slots * edge * edge + 4 * stage_size * edge * 128
        + 12 * size_y * size_x + 8 * len(growth) * cells_y * cells_x
    )
    return pl.pallas_call(
        functools.partial(exchange_kernel, span_x, span_y, growth, capacity),
        in_specs=[anywhere] + [inside] * 10,
        out_specs=[anywhere] * 2 + [inside] * 2,
        out_shape=[
            jax.ShapeDtypeStruct(log_crit.shape, jnp.float32),
            jax.ShapeDtypeStruct((steps, group, cells_y, cells_x), jnp.float32),
            jax.ShapeDtypeStruct((8, 128), jnp.float32),
            jax.ShapeDtypeStruct((8, 128), jnp.float32),
        ],
        scratch_shapes=[
            pltpu.VMEM(log_crit.shape, jnp.float32),
            pltpu.VMEM((steps, group, cells_y, cells_x), jnp.float32),
            pltpu.VMEM(table.shape, jnp.float32),
            pltpu.VMEM((2 * len(growth), cells_y, cells_x), jnp.float32),
            pltpu.VMEM((bins.shape[0], cells_y, cells_x), jnp.float32),
            parts,
            parts,
            planes,
            planes,
            packing,
            packing,
            pltpu.VMEM((stage_size, edge, 128), jnp.float32),
            halved,
            halved,
            pltpu.VMEM((span_x * span_y, 8, 128), jnp.float32),
            pltpu.VMEM((2, 2 * bins.shape[0], every), jnp.int32),
            pltpu.SMEM((2 * bins.shape[0], every), jnp.int32),
            pltpu.SMEM((2 * bins.shape[0], every), jnp.int32),
            pltpu.SemaphoreType.DMA((4,)),
            pltpu.SemaphoreType.DMA,
            pltpu.SemaphoreType.DMA((5,)),
        ]
        + [sems] * 10
        + [pltpu.SemaphoreType.DMA((3,))],
        compiler_params=pltpu.CompilerParams(
            collective_id=collective, has_side_effects=True,
            vmem_limit_bytes=min(held + held // 16 + 2 * 1024 * 1024, vmem_grant),
        ),
        name=f"exchange{slots}",
    )(
        log_crit, bins, live, routes, table, rise, mask, cy_high, cy_low, cx_high, cx_low,
    )


def turned(value):
    flat = jnp.swapaxes(value, 0, 1)
    return jnp.swapaxes(jnp.stack([flat[r].T for r in range(8)]), 0, 1)


def turn_kernel(source_ref, kept_ref, out_ref, kept_out):
    for row in range(0, source_ref.shape[1], 8):
        out_ref[:, row : row + 8, :] = turned(source_ref[:, row : row + 8, :])
    kept_out[...] = kept_ref[...]


def turn(source, kept):
    depth_all, cells_y, cells_x = source.shape
    rows = 8
    planes = pl.BlockSpec((depth_all, rows, cells_x), lambda j: (0, j, 0))
    cells = pl.BlockSpec((cells_x, rows, depth_all), lambda j: (0, j, 0))
    shape = jax.ShapeDtypeStruct((cells_x, cells_y, depth_all), jnp.float32)
    return pl.pallas_call(
        turn_kernel,
        grid=(cells_y // rows,),
        in_specs=[planes, cells],
        out_specs=[cells, cells],
        out_shape=[shape, shape],
        compiler_params=pltpu.CompilerParams(vmem_limit_bytes=16 * 1024 * 1024),
        name="turn",
    )(source, kept)


def wave_freq(length):
    half = length // 2
    return np.concatenate([np.arange(half + 1), np.arange(1, half)])


def wave_table(length):
    indices = np.arange(length)
    turns = indices[:, None] * wave_freq(length)[None, :] % length
    shift = np.where(indices < length // 2 + 1, 0.0, math.pi / 2)[None, :]
    return jnp.asarray(np.cos(2.0 * math.pi / length * turns - shift), jnp.float32)


def circulant(gain, table):
    length = gain.shape[0]
    half = length // 2
    freq = wave_freq(length)
    weight = jnp.concatenate([gain[: half + 1], gain[1:half]])
    doubled = jnp.asarray(np.where((freq == 0) | (freq == half), 1.0, 2.0), jnp.float32)
    scaled = lax.optimization_barrier(table * (weight * doubled / length))
    return lax.dot_general(
        scaled, table, (((1,), (1,)), ((), ())), precision=lax.Precision.HIGHEST
    )


def on_device(log_crit, col_bins, rate_table, tile_mask, tile_route, filt_x, filt_y):
    blocks_x, blocks_y, tiles = tile_mask.shape
    cells_x, cells_y, depth_all = log_crit.shape
    edge = cells_x // blocks_x
    span_x, span_y = lax.axis_size("gx"), lax.axis_size("gy")
    devices = span_x * span_y
    nodes = rate_table.shape[1]
    half = nodes // 2

    bins = col_bins.transpose(2, 1, 0)
    live = jnp.repeat((tile_mask == 1).astype(jnp.float32).transpose(2, 1, 0), edge, axis=2)
    routes = jnp.repeat(
        tile_route.transpose(2, 1, 0).reshape(tiles * blocks_y, blocks_x), edge, axis=1
    )
    table = jnp.concatenate([rate_table[:, half:], rate_table[:, half - 1 :: -1]], axis=1).T

    growth = node_growth(nodes)
    ends = np.array([growth, [1.0 / e for e in growth]], np.float32)
    rise = jnp.asarray(np.broadcast_to(ends[:, :, None], (2, half, table.shape[1])))
    capacity = blocks_x * blocks_y * tiles // 2
    table_x = wave_table(filt_x.shape[0])
    table_y = table_x if filt_y.shape == filt_x.shape else wave_table(filt_y.shape[0])
    mask = (tile_mask == 1).astype(jnp.float32).reshape(1, -1)
    mask = jnp.pad(mask, ((0, 7), (0, 128 - mask.shape[1])))
    every = span_y * blocks_y // 2 * span_x * blocks_x
    few = every * 19 // 32
    operands = (
        log_crit, bins, live, routes, table, rise, mask,
        *outer_halves(circulant(filt_y, table_y)), *outer_halves(circulant(filt_x, table_x)),
    )

    def run(slots, collective):
        return exchange(slots, collective, span_x, span_y, growth, capacity, *operands)

    def finish(planes, recomb):
        return turn(planes.reshape(depth_all, cells_y, cells_x), recomb)

    recomb, back, device_load, most = run(few, 2)
    smoothed, recomb = lax.cond(
        most[0, 0] <= few, finish, lambda planes, cells: finish(run(every, 3)[1], cells), back, recomb
    )
    return (recomb, smoothed, device_load[:1, :1])


def solution(mesh):
    placed = (
        P("gx", "gy", None),
        P("gx", "gy", None),
        P(),
        P("gx", "gy", None),
        P("gx", "gy", None),
        P(),
        P(),
    )
    return jax.shard_map(
        on_device,
        mesh=mesh,
        in_specs=placed,
        out_specs=(P("gx", "gy", None), P("gx", "gy", None), P("gx", "gy")),
        check_vma=False,
    )
```
